32 devices in a mesh: fsdp: 8 (over z, y), tensor: 4 (over x, core).
Axes of the slice: x: 2, y: 2, z: 4, core: 2. Of those that a mesh axis runs over, the one named last changes fastest.
Arguments:
- activations: bfloat16 [8192, 5120], P('fsdp', 'tensor'), may hold values from -6 to 6
- cotangent: bfloat16 [8192, 5120], P('fsdp', 'tensor'), may hold values from -0.06591797 to 0.06591797
- weights: float32 [5120, 5120], P(None, ('tensor', 'fsdp')), may hold values from -0.025 to 0.025
- first_moment: float32 [5120, 5120], P(None, ('tensor', 'fsdp')), may hold values from -3 to 3
- second_moment: float32 [5120, 5120], P(None, ('tensor', 'fsdp')), may hold values from 0.01 to 1
Outputs:
- weights_new: float32 [5120, 5120], P('fsdp', 'tensor')
- first_new: float32 [5120, 5120], P('fsdp', 'tensor')
- second_new: float32 [5120, 5120], P('fsdp', 'tensor')
- weights_bf16: bfloat16 [5120, 5120], P(None, 'tensor')
The draws below stay inside these ranges and needn't reach their ends.
All inputs are finite; a program needn't handle non-finite values.
Results may differ from the reference program's by a relative error of at most 0.014.
Values may be sent and summed in bfloat16 or wider, within the bound.
A program may use at most 128 MiB of HBM per device.

```python
import math
import jax
import jax.numpy as jnp
from jax import lax

D = 5120
TOK_DEV = 1024
STEP = 20
TOKENS = 8192
N_FSDP = 8


def with_spikes(array, key, source, target, parts, factor):
    owner, partner = [(jnp.arange(array.shape[dim]) // (array.shape[dim] // parts)).reshape([-1 if axis == dim else 1 for axis in range(array.ndim)]) for dim in (source, target)]
    chosen = jax.random.permutation(key, parts)[partner]
    strong = (owner == chosen) | (owner == (partner + parts // 2) % parts)
    return jnp.where(strong, factor * array, array)


def block_levels(key, extent, split, low, largest):
    factor_of = 1.0
    for dim, blocks in split:
        heights = jax.random.uniform(jax.random.fold_in(jax.random.fold_in(key, 6), dim), (blocks,), jnp.float32, low / len(split), largest / len(split))
        factor_of = factor_of * jnp.repeat(jnp.exp(heights), extent[dim] // blocks).reshape((-1,) + (1,) * (len(extent) - 1 - dim))
    return factor_of


def normal_values(stream_key, extent, scale, most, pieces=(), kind=jnp.bfloat16):
    array = scale * jax.random.normal(stream_key, extent, jnp.float32)
    if pieces:
        array = array * block_levels(stream_key, extent, pieces, -0.22, 0.18)
    return jnp.clip(array, -most, most).astype(kind)


def heavy_noise(own_key, dims, deviation, reach, split, heavy, dtype=jnp.bfloat16):
    values = deviation * jax.random.normal(own_key, dims, jnp.float32)
    if split:
        values = values * block_levels(own_key, dims, split, -0.22, 0.18)
    return jnp.clip(with_spikes(values, jax.random.fold_in(own_key, 3), *heavy), -reach, reach).astype(dtype)


def setup_inputs(seed: int = 0) -> dict:
    arg_keys = jax.random.split(jax.random.key(seed), 6)
    activations = heavy_noise(arg_keys[0], (TOKENS, D), 1.0, 6.0, ((0, 8), (1, 4)), (0, 1, 8, 2.0))
    cotangent = normal_values(arg_keys[1], (TOKENS, D), (1.0 / TOKENS ** 0.5), 0.06591797, ((0, 8), (1, 4)))
    weights = normal_values(arg_keys[2], (D, D), 0.004, 0.025, ((1, 32),), jnp.float32)
    first_moment = normal_values(arg_keys[3], (D, D), 0.5, 3.0, ((1, 32),), jnp.float32)
    second_moment = jnp.clip(jnp.exp(math.log(1.0) - 4.6051702 * jax.random.uniform(arg_keys[4], (D, D), jnp.float32) ** block_levels(arg_keys[4], (D, D), ((1, 32),), -0.2, 0.2)), 0.01, 1.0)
    return {"activations": activations, "cotangent": cotangent, "weights": weights, "first_moment": first_moment, "second_moment": second_moment}


beta_one = 0.9
beta_two = 0.95
adam_eps = 1e-08
learn_rate = 0.0003
decay_rate = 0.1

def adam_update(weights, first_moment, second_moment, gradient):
    first_new = beta_one * first_moment + (1.0 - beta_one) * gradient
    second_new = beta_two * second_moment + (1.0 - beta_two) * gradient * gradient
    corrected = first_new / (1.0 - beta_one ** STEP)
    scaled = jnp.sqrt(second_new / (1.0 - beta_two ** STEP)) + adam_eps
    weights_new = weights - learn_rate * (corrected / scaled + decay_rate * weights)
    return (weights_new, first_new, second_new)

def reference(activations, cotangent, weights, first_moment, second_moment):
    token_blocks = activations.reshape(N_FSDP, TOK_DEV, D)
    cotangent_blocks = cotangent.reshape(N_FSDP, TOK_DEV, D)

    def accumulate(running, block_pair):
        product = lax.dot_general(block_pair[0].astype(jnp.float32), block_pair[1].astype(jnp.float32), (((0,), (0,)), ((), ())))
        rounded = lax.optimization_barrier(product.astype(jnp.bfloat16))
        return (running + rounded.astype(jnp.float32), None)
    gradient, unused = lax.scan(accumulate, jnp.zeros((D, D), jnp.float32), (token_blocks, cotangent_blocks))
    weights_new, first_new, second_new = adam_update(weights, first_moment, second_moment, gradient)
    return (weights_new, first_new, second_new, weights_new.astype(jnp.bfloat16))
```

```python
import functools

import jax
import jax.numpy as jnp
from jax import lax
from jax.experimental import pallas as pl
from jax.experimental.pallas import tpu as pltpu
from jax.sharding import PartitionSpec as P


STEP = 20


beta_one = 0.9
beta_two = 0.95
adam_eps = 1e-08
learn_rate = 0.0003
decay_rate = 0.1


def adam_update(weights, first_moment, second_moment, gradient):
    first_new = beta_one * first_moment + (1.0 - beta_one) * gradient
    second_new = beta_two * second_moment + (1.0 - beta_two) * gradient * gradient
    corrected = first_new / (1.0 - beta_one**STEP)
    scaled = jnp.sqrt(second_new / (1.0 - beta_two**STEP)) + adam_eps
    weights_new = weights - learn_rate * (corrected / scaled + decay_rate * weights)
    return (weights_new, first_new, second_new)


def line_pairs(length, step, senders):
    return [
        (2 * z + p, 2 * (z + step) + p)
        for z in range(length)
        for p in range(2)
        if senders(z) and 0 <= z + step < length
    ]


def reduce_line(term, z, length):
    last = length - 1
    right = left = None
    for s in range(last):
        up = term(jnp.clip(last + z - s, 0, last))
        down = term(jnp.clip(s - last + z, 0, last))
        if s:
            up = (up.astype(jnp.float32) + right.astype(jnp.float32)).astype(jnp.bfloat16)
            down = (down.astype(jnp.float32) + left.astype(jnp.float32)).astype(jnp.bfloat16)
        right = lax.ppermute(up, "fsdp", line_pairs(length, 1, lambda i: i <= s))
        left = lax.ppermute(down, "fsdp", line_pairs(length, -1, lambda i: i >= last - s))
    own = term(z)
    own = own.astype(jnp.float32)
    if last:
        own = own + right.astype(jnp.float32) + left.astype(jnp.float32)
    return own


def gather_kernel(
    length, own_ref, out_ref, local_sem, y_send, y_recv, r_send, r_recv, l_send, l_recv
):
    f = lax.axis_index("fsdp")
    z, p = f // 2, f % 2
    last = length - 1
    rows = own_ref.shape[0]
    pair, right, left = f + 1 - 2 * p, f + 2, f - 2

    def block(c):
        return out_ref.at[pl.ds((2 * c + p) * rows, rows)]

    def copy(src, dst, send, recv, target):
        return pltpu.make_async_remote_copy(
            src_ref=src,
            dst_ref=dst,
            send_sem=send,
            recv_sem=recv,
            device_id={"fsdp": target},
            device_id_type=pl.DeviceIdType.MESH,
        )

    def to_pair(c, src=None):
        return copy(block(c) if src is None else src, block(c), y_send.at[c], y_recv.at[c], pair)

    def to_right(s, src=None):
        c = z - s
        return copy(block(c) if src is None else src, block(c), r_send.at[s], r_recv.at[s], right)

    def to_left(s, src=None):
        c = z + s
        return copy(block(c) if src is None else src, block(c), l_send.at[s], l_recv.at[s], left)

    barrier = pltpu.get_barrier_semaphore()
    pl.semaphore_signal(
        barrier, inc=1, device_id={"fsdp": pair}, device_id_type=pl.DeviceIdType.MESH
    )

    @pl.when(z > 0)
    def _():
        pl.semaphore_signal(
            barrier, inc=1, device_id={"fsdp": left}, device_id_type=pl.DeviceIdType.MESH
        )

    @pl.when(z < last)
    def _():
        pl.semaphore_signal(
            barrier, inc=1, device_id={"fsdp": right}, device_id_type=pl.DeviceIdType.MESH
        )

    span = max(last, 1)
    pl.semaphore_wait(barrier, 1 + (z + span - 1) // span + (last - z + span - 1) // span)

    @pl.when(z < last)
    def _():
        to_right(0, own_ref).start()

    @pl.when(z > 0)
    def _():
        to_left(0, own_ref).start()

    to_pair(z, own_ref).start()
    here = pltpu.make_async_copy(own_ref, block(z), local_sem)
    here.start()

    for s in range(last):

        @pl.when(z > s)
        def _():
            c = z - 1 - s
            copy(block(c), block(c), r_send.at[s], r_recv.at[s], left).wait_recv()
            if s + 1 < last:

                @pl.when(z < last)
                def _():
                    to_right(s + 1).start()

            to_pair(c).start()

        @pl.when(z < last - s)
        def _():
            c = z + 1 + s
            copy(block(c), block(c), l_send.at[s], l_recv.at[s], right).wait_recv()
            if s + 1 < last:

                @pl.when(z > 0)
                def _():
                    to_left(s + 1).start()

            to_pair(c).start()

    for s in range(last):

        @pl.when((z < last) & (z >= s))
        def _():
            to_right(s).wait_send()

        @pl.when((z > 0) & (last - z >= s))
        def _():
            to_left(s).wait_send()

    here.wait()
    for c in range(length):
        to_pair(c).wait_send()
        theirs = out_ref.at[pl.ds((2 * c + 1 - p) * rows, rows)]
        copy(theirs, theirs, y_send.at[c], y_recv.at[c], pair).wait_recv()


def gather_line(own, length):
    rows, cols = own.shape
    dma = pltpu.SemaphoreType.DMA
    steps = max(length - 1, 1)
    return pl.pallas_call(
        functools.partial(gather_kernel, length),
        out_shape=jax.ShapeDtypeStruct((2 * length * rows, cols), own.dtype),
        in_specs=[pl.BlockSpec(memory_space=pltpu.VMEM)],
        out_specs=pl.BlockSpec(memory_space=pl.ANY),
        scratch_shapes=[dma, dma((length,)), dma((length,))] + [dma((steps,))] * 4,
        compiler_params=pltpu.CompilerParams(collective_id=0, has_side_effects=True),
        name="gather_rows",
    )(own)


def body(activations, cotangent, weights, first_moment, second_moment, *, n, parts):
    f = lax.axis_index("fsdp")
    z, p = f // 2, f % 2
    length = n // 2
    depth, cols = weights.shape
    rows = depth // n
    tok, width = activations.shape
    pair = [(i, i ^ 1) for i in range(n)]

    packed = jnp.concatenate([weights, first_moment, second_moment], axis=1).astype(jnp.bfloat16)
    lines = [[2 * i + q for i in range(length)] for q in range(2)]
    packed = lax.optimization_barrier(packed.reshape(length, 2, rows, 3 * cols))
    along = lax.all_to_all(packed, "fsdp", 0, 0, axis_index_groups=lines)
    blocks = activations.reshape(tok, width // (2 * rows), 2, rows)
    keep = lax.dynamic_index_in_dim(blocks, p, 2, False).reshape(tok, width // 2)
    give = lax.dynamic_index_in_dim(blocks, 1 - p, 2, False).reshape(tok, width // 2)
    got = lax.ppermute(give, "fsdp", pair)
    cot_peer = lax.ppermute(cotangent, "fsdp", pair)
    mine = lax.all_gather(keep, "tensor")
    theirs = lax.all_gather(got, "tensor")

    def product(a, b):
        return lax.dot_general(a, b, (((0,), (0,)), ((), ())), preferred_element_type=jnp.float32)

    groups = length // parts

    def term(c):
        at = (c // groups, 0, (c % groups) * rows)
        near, far = (
            lax.dynamic_slice(array, at, (1, tok, rows))[0] for array in (mine, theirs)
        )
        total = product(near, cotangent) + product(far, cot_peer)
        return lax.optimization_barrier(total.astype(jnp.bfloat16))

    gradient = reduce_line(term, z, length)

    stay = lax.dynamic_index_in_dim(along, p, 1, False)
    across = lax.ppermute(lax.dynamic_index_in_dim(along, 1 - p, 1, False), "fsdp", pair)
    moved = jnp.where(p == 0, jnp.stack([stay, across], 1), jnp.stack([across, stay], 1))

    def owned(k):
        pieces = [moved[i // 2, i % 2, :, k * cols : (k + 1) * cols] for i in range(n)]
        return lax.optimization_barrier(jnp.concatenate(pieces, axis=1)).astype(jnp.float32)

    weights_new, first_new, second_new = adam_update(owned(0), owned(1), owned(2), gradient)
    rounded = weights_new.astype(jnp.bfloat16)
    weights_bf16 = gather_line(rounded, length)
    return (weights_new, first_new, second_new, weights_bf16)


CHUNKS = 2
LANE = 128


def fsdp_kernel(
    n, parts, chunks, act, cot, w_in, m_in, v_in, w_out, m_out, v_out, b_out,
    a_buf, at_buf, c_buf, st_in, st_out, fin, stg, up, dn, tmp, stage, wb,
    loc_sem, st_sem, out_sem, own_sem, give_s, give_r, cot_s, cot_r,
    t_send, t_recv, fin_s, fin_r, stg_s, stg_r, fwd_s, fwd_r,
    up_s, up_r, dn_s, dn_r, y_send, y_recv, r_send, r_recv, l_send, l_recv,
):
    f = lax.axis_index("fsdp")
    t = lax.axis_index("tensor")
    z, p = f // 2, f % 2
    length = n // 2
    last = length - 1
    rows, width = a_buf.shape[-1], act.shape[1]
    cols = w_in.shape[1]
    part = rows // chunks
    pair = f + 1 - 2 * p
    bits = [b for b in (1 << i for i in range(parts.bit_length()))][::-1]
    bits = [b for b in bits if b < parts]

    def copy(src, dst, send, recv, axis, target):
        return pltpu.make_async_remote_copy(
            src_ref=src, dst_ref=dst, send_sem=send, recv_sem=recv,
            device_id={axis: target}, device_id_type=pl.DeviceIdType.MESH,
        )

    def flip(b):
        return t + b - 2 * b * ((t // b) % 2)

    barrier = pltpu.get_barrier_semaphore()

    def greet(axis, target):
        pl.semaphore_signal(
            barrier, inc=1, device_id={axis: target}, device_id_type=pl.DeviceIdType.MESH
        )

    greet("fsdp", pair)
    for j in range(1, length):
        greet("fsdp", ((z + j) % length) * 2 + p)
    for b in bits:
        greet("tensor", flip(b))
    pl.semaphore_wait(barrier, length + len(bits))

    def feature(q):
        return act.at[:, pl.ds(pl.multiple_of(q * rows, rows), rows)]

    give = copy(feature(1 - p), a_buf.at[1, t], give_s, give_r, "fsdp", pair)
    give.start()
    cots = copy(cot, c_buf.at[1], cot_s, cot_r, "fsdp", pair)
    cots.start()
    mine = pltpu.make_async_copy(feature(p), a_buf.at[0, t], loc_sem.at[0])
    mine.start()
    here = pltpu.make_async_copy(cot, c_buf.at[0], loc_sem.at[1])
    here.start()

    def held(i):
        found = [t]
        for b in bits[:i]:
            found = found + [h + b - 2 * b * ((t // b) % 2) for h in found]
        return found

    def block_copy(which, i, h):
        return copy(
            a_buf.at[which, h], a_buf.at[which, h], t_send.at[which, i, h],
            t_recv.at[which, h], "tensor", flip(bits[i]),
        )

    def spread_own(which):
        for i in range(len(bits)):
            block_copy(which, i, t).start()

    def spread_round(which, i):
        b = bits[i]
        for h in held(i):
            g = h + b - 2 * b * ((t // b) % 2)
            block_copy(which, i, g).wait_recv()
            for j in range(i + 1, len(bits)):
                block_copy(which, j, g).start()

    def spread_done(which):
        for i in range(len(bits)):
            for h in held(i):
                block_copy(which, i, h).wait_send()

    mine.wait()
    spread_own(0)

    def load_state(i, slot):
        at = pl.ds(pl.multiple_of((i % n) * rows + (i // n) * part, part), part)
        return [
            pltpu.make_async_copy(src.at[at], st_in.at[slot, a], st_sem.at[slot, a])
            for a, src in enumerate((w_in, m_in, v_in))
        ]

    def span(k):
        return pl.ds(pl.multiple_of(k * part, part), part)

    def fin_copy(k, zs, zd):
        return copy(
            st_out.at[2 * zd + p, span(k)], fin.at[2 * zs + p, span(k)],
            fin_s.at[k, zd], fin_r.at[k, zs], "fsdp", 2 * zd + p,
        )

    def stg_copy(k, zs, zd):
        return copy(
            st_out.at[2 * zd + 1 - p, span(k)], stg.at[zs, span(k)],
            stg_s.at[k, zd], stg_r.at[k, zs], "fsdp", 2 * zd + p,
        )

    for c in load_state(0, 0):
        c.start()

    def pack(i, carry):
        slot = i % 2

        @pl.when(i + 1 < chunks * n)
        def _():
            for c in load_state(i + 1, (i + 1) % 2):
                c.start()

        for c in load_state(i, slot):
            c.wait()
        d, k = i % n, i // n
        for a in range(3):
            st_out[d, span(k), a * cols : (a + 1) * cols] = st_in[slot, a].astype(jnp.bfloat16)

        @pl.when(d == f)
        def _():
            fin[d, span(k), :] = st_out[d, span(k), :]

        zd = d // 2

        @pl.when((zd != z) & (d % 2 == p))
        def _():
            fin_copy(k, z, zd).start()

        @pl.when((zd != z) & (d % 2 != p))
        def _():
            stg_copy(k, z, zd).start()

        return carry

    lax.fori_loop(0, chunks * n, pack, 0)

    def turn(which):
        def tile(i, carry):
            j, r = i // (rows // LANE), i % (rows // LANE)
            at = pl.ds(pl.multiple_of(r * LANE, LANE), LANE)
            at_buf[which, j, at, :] = a_buf[which, j, :, at].T
            return carry

        lax.fori_loop(0, parts * (rows // LANE), tile, 0)

    give.wait_recv()
    spread_own(1)
    for i in range(len(bits)):
        spread_round(0, i)
    turn(0)
    for i in range(len(bits)):
        spread_round(1, i)
    turn(1)

    def forward(k, zs):
        src = stg.at[zs, span(k)]
        return copy(
            src, fin.at[2 * zs + p, span(k)], fwd_s.at[k, zs], fwd_r.at[k, zs], "fsdp", pair
        )

    def forward_own(k):
        return copy(
            st_out.at[pair, span(k)], fin.at[f, span(k)],
            fwd_s.at[k, z], fwd_r.at[k, z], "fsdp", pair,
        )

    here.wait()
    cots.wait()

    def forward_state(k):
        forward_own(k).start()
        for j in range(1, length):
            zs = (z + j) % length
            stg_copy(k, zs, z).wait_recv()
            forward(k, zs).start()

    def state_here(k):
        for j in range(1, length):
            fin_copy(k, (z + j) % length, z).wait_recv()
        for zs in range(length):
            copy(
                stg.at[zs, span(k)], fin.at[2 * zs + 1 - p, span(k)],
                fwd_s.at[k, zs], fwd_r.at[k, zs], "fsdp", pair,
            ).wait_recv()

    block_n = 2 * LANE

    def term(d, k):
        def tile(i, carry):
            at = pl.ds(pl.multiple_of(i * block_n, block_n), block_n)
            total = jnp.dot(
                at_buf[0, d, span(k), :], c_buf[0, :, at], preferred_element_type=jnp.float32
            ) + jnp.dot(
                at_buf[1, d, span(k), :], c_buf[1, :, at], preferred_element_type=jnp.float32
            )
            tmp[:, at] = total
            return carry

        lax.fori_loop(0, width // block_n, tile, 0)

    def send_up(k, s):
        slot = s - jnp.minimum(z, 1)
        return copy(up.at[k, slot], up.at[k, s], up_s.at[k, s], up_r.at[k, s], "fsdp", f + 2)

    def send_dn(k, s):
        slot = s - jnp.minimum(last - z, 1)
        return copy(dn.at[k, slot], dn.at[k, s], dn_s.at[k, s], dn_r.at[k, s], "fsdp", f - 2)

    def take_up(k, s):
        copy(up.at[k, s], up.at[k, s], up_s.at[k, s], up_r.at[k, s], "fsdp", f - 2).wait_recv()

    def take_dn(k, s):
        copy(dn.at[k, s], dn.at[k, s], dn_s.at[k, s], dn_r.at[k, s], "fsdp", f + 2).wait_recv()

    def add_in(ref, k, slot, first):
        @pl.when(first)
        def _():
            ref[k, slot] = tmp[...].astype(jnp.bfloat16)

        @pl.when(jnp.logical_not(first))
        def _():
            ref[k, slot] = (tmp[...] + ref[k, slot].astype(jnp.float32)).astype(jnp.bfloat16)

    def reduce_step(k, s):
        @pl.when(z <= s)
        def _():
            term(last + z - s, k)
            if s:

                @pl.when(z > 0)
                def _():
                    take_up(k, s - 1)

            add_in(up, k, s - jnp.minimum(z, 1), z == 0)
            send_up(k, s).start()

        @pl.when(z >= last - s)
        def _():
            term(s - last + z, k)
            if s:

                @pl.when(z < last)
                def _():
                    take_dn(k, s - 1)

            add_in(dn, k, s - jnp.minimum(last - z, 1), z == last)
            send_dn(k, s).start()

    sub = stage.shape[2]
    subs = part // sub

    def out_copies(i, slot):
        at = pl.ds(pl.multiple_of(i * sub, sub), sub)
        return [
            pltpu.make_async_copy(stage.at[slot, a], dst.at[at], out_sem.at[slot, a])
            for a, dst in enumerate((w_out, m_out, v_out))
        ]

    def adam(k):
        term(z, k)

        @pl.when(z > 0)
        def _():
            take_up(k, last - 1)
            tmp[...] += up[k, last - 1].astype(jnp.float32)

        @pl.when(z < last)
        def _():
            take_dn(k, last - 1)
            tmp[...] += dn[k, last - 1].astype(jnp.float32)

        state_here(k)

        def piece(j, carry):
            i = k * subs + j
            slot = i % 2

            @pl.when(i >= 2)
            def _():
                for c in out_copies(i - 2, slot):
                    c.wait()

            at = pl.ds(pl.multiple_of(i * sub, sub), sub)
            loc = pl.ds(pl.multiple_of(j * sub, sub), sub)
            state = [fin[src, at, :].astype(jnp.float32) for src in range(n)]
            old = [
                jnp.concatenate([x[:, a * cols : (a + 1) * cols] for x in state], axis=1)
                for a in range(3)
            ]
            new = adam_update(*old, tmp[loc, :])
            for a in range(3):
                stage[slot, a] = new[a]
            wb[k, loc, :] = new[0].astype(jnp.bfloat16)
            for c in out_copies(i, slot):
                c.start()
            return carry

        lax.fori_loop(0, subs, piece, 0)

    def block(c, q, k):
        return b_out.at[pl.ds(pl.multiple_of((2 * c + q) * rows + k * part, part), part)]

    def to_pair(k, c, src=None):
        src = block(c, p, k) if src is None else src
        return copy(src, block(c, p, k), y_send.at[k, c], y_recv.at[k, c], "fsdp", pair)

    def to_right(k, s, src=None):
        src = block(z - s, p, k) if src is None else src
        return copy(
            src, block(z - s, p, k), r_send.at[k, s], r_recv.at[k, s], "fsdp", f + 2
        )

    def to_left(k, s, src=None):
        src = block(z + s, p, k) if src is None else src
        return copy(
            src, block(z + s, p, k), l_send.at[k, s], l_recv.at[k, s], "fsdp", f - 2
        )

    def keep(k):
        return pltpu.make_async_copy(wb.at[k], block(z, p, k), own_sem.at[k])

    def gather_start(k):
        to_pair(k, z, wb.at[k]).start()

        @pl.when(z < last)
        def _():
            to_right(k, 0, wb.at[k]).start()

        @pl.when(z > 0)
        def _():
            to_left(k, 0, wb.at[k]).start()

        keep(k).start()

    def gather_step(k, s):
        @pl.when(z > s)
        def _():
            c = z - 1 - s
            got = block(c, p, k)
            copy(got, got, r_send.at[k, s], r_recv.at[k, s], "fsdp", f - 2).wait_recv()
            if s + 1 < last:

                @pl.when(z < last)
                def _():
                    to_right(k, s + 1).start()

            to_pair(k, c).start()

        @pl.when(z < last - s)
        def _():
            c = z + 1 + s
            got = block(c, p, k)
            copy(got, got, l_send.at[k, s], l_recv.at[k, s], "fsdp", f + 2).wait_recv()
            if s + 1 < last:

                @pl.when(z > 0)
                def _():
                    to_left(k, s + 1).start()

            to_pair(k, c).start()

    forward_state(0)
    for s in range(last):
        reduce_step(0, s)
    for k in range(1, chunks):
        forward_state(k)
        reduce_step(k, 0)
        adam(k - 1)
        gather_start(k - 1)
        for s in range(1, last):
            reduce_step(k, s)
            gather_step(k - 1, s - 1)
        if last > 1:
            gather_step(k - 1, last - 1)
    adam(chunks - 1)
    gather_start(chunks - 1)
    for s in range(last):
        gather_step(chunks - 1, s)

    give.wait_send()
    spread_done(0)
    spread_done(1)
    for j in (2, 1):
        for c in out_copies(chunks * subs - j, (chunks * subs - j) % 2):
            c.wait()
    for k in range(chunks):
        keep(k).wait()
        for j in range(1, length):
            zd = (z + j) % length
            fin_copy(k, z, zd).wait_send()
            stg_copy(k, z, zd).wait_send()
        for zs in range(length):
            forward(k, zs).wait_send()
        for s in range(last):

            @pl.when(z <= s)
            def _():
                send_up(k, s).wait_send()

            @pl.when(z >= last - s)
            def _():
                send_dn(k, s).wait_send()

            @pl.when((z < last) & (z >= s))
            def _():
                to_right(k, s).wait_send()

            @pl.when((z > 0) & (last - z >= s))
            def _():
                to_left(k, s).wait_send()

        for c in range(length):
            to_pair(k, c).wait_send()
            theirs = block(c, 1 - p, k)
            copy(theirs, theirs, y_send.at[k, c], y_recv.at[k, c], "fsdp", pair).wait_recv()


def fast_body(activations, cotangent, weights, first_moment, second_moment, *, n, parts):
    depth, cols = weights.shape
    tok, width = activations.shape
    rows = depth // n
    length, chunks = n // 2, CHUNKS
    part = rows // chunks
    sub = part // 4
    rounds = parts.bit_length() - 1
    dma = pltpu.SemaphoreType.DMA
    half, full = jnp.bfloat16, jnp.float32
    hops = max(length - 1, 1)
    row = jax.ShapeDtypeStruct((rows, width), full)
    anywhere = pl.BlockSpec(memory_space=pl.ANY)
    return tuple(
        pl.pallas_call(
            functools.partial(fsdp_kernel, n, parts, chunks),
            out_shape=(row, row, row, jax.ShapeDtypeStruct((depth, width), half)),
            in_specs=[anywhere] * 5,
            out_specs=(anywhere,) * 4,
            scratch_shapes=[
                pltpu.VMEM((2, parts, tok, rows), half),
                pltpu.VMEM((2, parts, rows, tok), half),
                pltpu.VMEM((2, tok, width), half),
                pltpu.VMEM((2, 3, part, cols), full),
                pltpu.VMEM((n, rows, 3 * cols), half),
                pltpu.VMEM((n, rows, 3 * cols), half),
                pltpu.VMEM((length, rows, 3 * cols), half),
                pltpu.VMEM((chunks, hops, part, width), half),
                pltpu.VMEM((chunks, hops, part, width), half),
                pltpu.VMEM((part, width), full),
                pltpu.VMEM((2, 3, sub, width), full),
                pltpu.VMEM((chunks, part, width), half),
                dma((2,)), dma((2, 3)), dma((2, 3)), dma((chunks,)),
                dma, dma, dma, dma,
                dma((2, rounds, parts)), dma((2, parts)),
            ]
            + [dma((chunks, length))] * 6
            + [dma((chunks, hops))] * 4
            + [dma((chunks, length))] * 2
            + [dma((chunks, hops))] * 4,
            compiler_params=pltpu.CompilerParams(
                collective_id=0, has_side_effects=True, vmem_limit_bytes=67043328
            ),
            name="fsdp_step",
        )(activations, cotangent, weights, first_moment, second_moment)
    )


def solution(mesh):
    n, parts = mesh.shape["fsdp"], mesh.shape["tensor"]

    def run(*arrays):
        rows, width = arrays[2].shape[0] // n, arrays[0].shape[1]
        fits = rows % LANE == 0 and rows % (64 * CHUNKS) == 0 and n == 2 * parts
        if fits and width == 2 * rows and parts & (parts - 1) == 0:
            return fast_body(*arrays, n=n, parts=parts)
        return body(*arrays, n=n, parts=parts)

    return jax.shard_map(
        run,
        mesh=mesh,
        in_specs=(
            P("fsdp", "tensor"),
            P("fsdp", "tensor"),
            P(None, ("tensor", "fsdp")),
            P(None, ("tensor", "fsdp")),
            P(None, ("tensor", "fsdp")),
        ),
        out_specs=(
            P("fsdp", "tensor"),
            P("fsdp", "tensor"),
            P("fsdp", "tensor"),
            P(None, "tensor"),
        ),
        check_vma=False,
    )
```

```python
import functools

import jax
import jax.numpy as jnp
from jax import lax
from jax.experimental import pallas as pl
from jax.experimental.pallas import tpu as pltpu
from jax.sharding import PartitionSpec as P


STEP = 20


beta_one = 0.9
beta_two = 0.95
adam_eps = 1e-08
learn_rate = 0.0003
decay_rate = 0.1


def adam_update(weights, first_moment, second_moment, gradient):
    first_new = beta_one * first_moment + (1.0 - beta_one) * gradient
    second_new = beta_two * second_moment + (1.0 - beta_two) * gradient * gradient
    corrected = first_new / (1.0 - beta_one**STEP)
    scaled = jnp.sqrt(second_new / (1.0 - beta_two**STEP)) + adam_eps
    weights_new = weights - learn_rate * (corrected / scaled + decay_rate * weights)
    return (weights_new, first_new, second_new)


def line_pairs(length, step, senders):
    return [
        (2 * z + p, 2 * (z + step) + p)
        for z in range(length)
        for p in range(2)
        if senders(z) and 0 <= z + step < length
    ]


def reduce_line(term, z, length):
    last = length - 1
    right = left = None
    for s in range(last):
        up = term(jnp.clip(last + z - s, 0, last))
        down = term(jnp.clip(s - last + z, 0, last))
        if s:
            up = (up.astype(jnp.float32) + right.astype(jnp.float32)).astype(jnp.bfloat16)
            down = (down.astype(jnp.float32) + left.astype(jnp.float32)).astype(jnp.bfloat16)
        right = lax.ppermute(up, "fsdp", line_pairs(length, 1, lambda i: i <= s))
        left = lax.ppermute(down, "fsdp", line_pairs(length, -1, lambda i: i >= last - s))
    own = term(z)
    own = own.astype(jnp.float32)
    if last:
        own = own + right.astype(jnp.float32) + left.astype(jnp.float32)
    return own


def gather_kernel(
    length, own_ref, out_ref, local_sem, y_send, y_recv, r_send, r_recv, l_send, l_recv
):
    f = lax.axis_index("fsdp")
    z, p = f // 2, f % 2
    last = length - 1
    rows = own_ref.shape[0]
    pair, right, left = f + 1 - 2 * p, f + 2, f - 2

    def block(c):
        return out_ref.at[pl.ds((2 * c + p) * rows, rows)]

    def copy(src, dst, send, recv, target):
        return pltpu.make_async_remote_copy(
            src_ref=src,
            dst_ref=dst,
            send_sem=send,
            recv_sem=recv,
            device_id={"fsdp": target},
            device_id_type=pl.DeviceIdType.MESH,
        )

    def to_pair(c, src=None):
        return copy(block(c) if src is None else src, block(c), y_send.at[c], y_recv.at[c], pair)

    def to_right(s, src=None):
        c = z - s
        return copy(block(c) if src is None else src, block(c), r_send.at[s], r_recv.at[s], right)

    def to_left(s, src=None):
        c = z + s
        return copy(block(c) if src is None else src, block(c), l_send.at[s], l_recv.at[s], left)

    barrier = pltpu.get_barrier_semaphore()
    pl.semaphore_signal(
        barrier, inc=1, device_id={"fsdp": pair}, device_id_type=pl.DeviceIdType.MESH
    )

    @pl.when(z > 0)
    def _():
        pl.semaphore_signal(
            barrier, inc=1, device_id={"fsdp": left}, device_id_type=pl.DeviceIdType.MESH
        )

    @pl.when(z < last)
    def _():
        pl.semaphore_signal(
            barrier, inc=1, device_id={"fsdp": right}, device_id_type=pl.DeviceIdType.MESH
        )

    span = max(last, 1)
    pl.semaphore_wait(barrier, 1 + (z + span - 1) // span + (last - z + span - 1) // span)

    @pl.when(z < last)
    def _():
        to_right(0, own_ref).start()

    @pl.when(z > 0)
    def _():
        to_left(0, own_ref).start()

    to_pair(z, own_ref).start()
    here = pltpu.make_async_copy(own_ref, block(z), local_sem)
    here.start()

    for s in range(last):

        @pl.when(z > s)
        def _():
            c = z - 1 - s
            copy(block(c), block(c), r_send.at[s], r_recv.at[s], left).wait_recv()
            if s + 1 < last:

                @pl.when(z < last)
                def _():
                    to_right(s + 1).start()

            to_pair(c).start()

        @pl.when(z < last - s)
        def _():
            c = z + 1 + s
            copy(block(c), block(c), l_send.at[s], l_recv.at[s], right).wait_recv()
            if s + 1 < last:

                @pl.when(z > 0)
                def _():
                    to_left(s + 1).start()

            to_pair(c).start()

    for s in range(last):

        @pl.when((z < last) & (z >= s))
        def _():
            to_right(s).wait_send()

        @pl.when((z > 0) & (last - z >= s))
        def _():
            to_left(s).wait_send()

    here.wait()
    for c in range(length):
        to_pair(c).wait_send()
        theirs = out_ref.at[pl.ds((2 * c + 1 - p) * rows, rows)]
        copy(theirs, theirs, y_send.at[c], y_recv.at[c], pair).wait_recv()


def gather_line(own, length):
    rows, cols = own.shape
    dma = pltpu.SemaphoreType.DMA
    steps = max(length - 1, 1)
    return pl.pallas_call(
        functools.partial(gather_kernel, length),
        out_shape=jax.ShapeDtypeStruct((2 * length * rows, cols), own.dtype),
        in_specs=[pl.BlockSpec(memory_space=pltpu.VMEM)],
        out_specs=pl.BlockSpec(memory_space=pl.ANY),
        scratch_shapes=[dma, dma((length,)), dma((length,))] + [dma((steps,))] * 4,
        compiler_params=pltpu.CompilerParams(collective_id=0, has_side_effects=True),
        name="gather_rows",
    )(own)


def body(activations, cotangent, weights, first_moment, second_moment, *, n, parts):
    f = lax.axis_index("fsdp")
    z, p = f // 2, f % 2
    length = n // 2
    depth, cols = weights.shape
    rows = depth // n
    tok, width = activations.shape
    pair = [(i, i ^ 1) for i in range(n)]

    packed = jnp.concatenate([weights, first_moment, second_moment], axis=1).astype(jnp.bfloat16)
    lines = [[2 * i + q for i in range(length)] for q in range(2)]
    packed = lax.optimization_barrier(packed.reshape(length, 2, rows, 3 * cols))
    along = lax.all_to_all(packed, "fsdp", 0, 0, axis_index_groups=lines)
    blocks = activations.reshape(tok, width // (2 * rows), 2, rows)
    keep = lax.dynamic_index_in_dim(blocks, p, 2, False).reshape(tok, width // 2)
    give = lax.dynamic_index_in_dim(blocks, 1 - p, 2, False).reshape(tok, width // 2)
    got = lax.ppermute(give, "fsdp", pair)
    cot_peer = lax.ppermute(cotangent, "fsdp", pair)
    mine = lax.all_gather(keep, "tensor")
    theirs = lax.all_gather(got, "tensor")

    def product(a, b):
        return lax.dot_general(a, b, (((0,), (0,)), ((), ())), preferred_element_type=jnp.float32)

    groups = length // parts

    def term(c):
        at = (c // groups, 0, (c % groups) * rows)
        near, far = (
            lax.dynamic_slice(array, at, (1, tok, rows))[0] for array in (mine, theirs)
        )
        total = product(near, cotangent) + product(far, cot_peer)
        return lax.optimization_barrier(total.astype(jnp.bfloat16))

    gradient = reduce_line(term, z, length)

    stay = lax.dynamic_index_in_dim(along, p, 1, False)
    across = lax.ppermute(lax.dynamic_index_in_dim(along, 1 - p, 1, False), "fsdp", pair)
    moved = jnp.where(p == 0, jnp.stack([stay, across], 1), jnp.stack([across, stay], 1))

    def owned(k):
        pieces = [moved[i // 2, i % 2, :, k * cols : (k + 1) * cols] for i in range(n)]
        return lax.optimization_barrier(jnp.concatenate(pieces, axis=1)).astype(jnp.float32)

    weights_new, first_new, second_new = adam_update(owned(0), owned(1), owned(2), gradient)
    rounded = weights_new.astype(jnp.bfloat16)
    weights_bf16 = gather_line(rounded, length)
    return (weights_new, first_new, second_new, weights_bf16)


LANE = 128


def fsdp_kernel(
    n, parts, sizes, act, cot, w_in, m_in, v_in, w_out, m_out, v_out, b_out,
    raw, give_t, at_buf, c_buf, st_in, st_out, fin, stg, up, dn, tmp, old, stage, wb,
    raw_sem, loc_sem, st_sem, out_sem, own_sem, give_s, give_r, cot_s, cot_r,
    t_send, t_recv, fin_s, fin_r, stg_s, stg_r, fwd_s, fwd_r,
    up_s, up_r, dn_s, dn_r, y_send, y_recv, r_send, r_recv, l_send, l_recv,
):
    f = lax.axis_index("fsdp")
    t = lax.axis_index("tensor")
    z, p = f // 2, f % 2
    length = n // 2
    last = length - 1
    tok, width = act.shape
    rows, cols = at_buf.shape[2], w_in.shape[0]
    pair = f + 1 - 2 * p
    bits = [1 << i for i in range(parts.bit_length() - 1)][::-1]
    starts = [sum(sizes[:k]) for k in range(len(sizes))]

    def copy(src, dst, send, recv, axis, target):
        return pltpu.make_async_remote_copy(
            src_ref=src, dst_ref=dst, send_sem=send, recv_sem=recv,
            device_id={axis: target}, device_id_type=pl.DeviceIdType.MESH,
        )

    def crossed(i, b):
        return i + b - 2 * b * ((t // b) % 2)

    def ring(j):
        return (z + j) % length

    def span(k):
        return pl.ds(starts[k], sizes[k])

    def lanes(i, size):
        return pl.ds(pl.multiple_of(i * size, size), size)

    def feature(q):
        return lanes(q, rows)

    raw_copies = [
        pltpu.make_async_copy(act.at[:, feature(q)], raw.at[i], raw_sem.at[i])
        for i, q in enumerate((1 - p, p))
    ]
    for c in raw_copies:
        c.start()
    here = pltpu.make_async_copy(cot, c_buf.at[0], loc_sem)
    here.start()

    def load_state(u, slot):
        d = 2 * ring(u + 1) + (p + 1 + u // length) % 2
        return [
            pltpu.make_async_copy(
                src.at[:, lanes(d, rows)], st_in.at[slot, a], st_sem.at[slot, a]
            )
            for a, src in enumerate((w_in, m_in, v_in))
        ]

    for c in load_state(0, 0):
        c.start()

    barrier = pltpu.get_barrier_semaphore()

    def greet(axis, target):
        pl.semaphore_signal(
            barrier, inc=1, device_id={axis: target}, device_id_type=pl.DeviceIdType.MESH
        )

    greet("fsdp", pair)
    for j in range(1, length):
        greet("fsdp", 2 * ring(j) + p)
    for b in bits:
        greet("tensor", crossed(t, b))
    pl.semaphore_wait(barrier, length + len(bits))

    head = tok // 4

    def cot_copy(i):
        at = pl.ds(0, head) if i == 0 else pl.ds(head, tok - head)
        return copy(cot.at[at], c_buf.at[1, at], cot_s.at[i], cot_r.at[i], "fsdp", pair)

    def turn(src, dst):
        def tile(r, carry):
            dst[lanes(r, LANE), :] = src[:, lanes(r, LANE)].T
            return carry

        lax.fori_loop(0, rows // LANE, tile, 0)

    def block_copy(which, i, h):
        return copy(
            at_buf.at[which, h], at_buf.at[which, h], t_send.at[which, i, h],
            t_recv.at[which, h], "tensor", crossed(t, bits[i]),
        )

    def held(i):
        found = [t]
        for b in bits[:i]:
            found = found + [crossed(h, b) for h in found]
        return found

    def spread_own(which):
        for i in range(len(bits)):
            block_copy(which, i, t).start()

    def spread_round(which, i):
        for h in held(i):
            g = crossed(h, bits[i])
            block_copy(which, i, g).wait_recv()
            for j in range(i + 1, len(bits)):
                block_copy(which, j, g).start()

    def spread_done(which):
        for i in range(len(bits)):
            for h in held(i):
                block_copy(which, i, h).wait_send()

    cot_copy(0).start()
    raw_copies[0].wait()
    turn(raw.at[0], give_t)
    give = copy(give_t, at_buf.at[1, t], give_s, give_r, "fsdp", pair)
    give.start()
    cot_copy(1).start()
    raw_copies[1].wait()
    turn(raw.at[1], at_buf.at[0, t])
    spread_own(0)

    def fin_copy(zs, zd):
        return copy(
            st_out.at[2 * zd + p], fin.at[2 * zs + p], fin_s.at[zd], fin_r.at[zs],
            "fsdp", 2 * zd + p,
        )

    def stg_copy(zs, zd):
        return copy(
            st_out.at[2 * zd + 1 - p], stg.at[zs], stg_s.at[zd], stg_r.at[zs],
            "fsdp", 2 * zd + p,
        )

    def pack(u, carry):
        slot = u % 2

        @pl.when(u + 1 < n)
        def _():
            for c in load_state(u + 1, (u + 1) % 2):
                c.start()

        for c in load_state(u, slot):
            c.wait()
        zd, q = ring(u + 1), (p + 1 + u // length) % 2
        d = 2 * zd + q
        for a in range(3):
            st_out[d, a * cols : (a + 1) * cols, :] = st_in[slot, a].astype(jnp.bfloat16)

        @pl.when(d == f)
        def _():
            fin[d] = st_out[d]

        @pl.when((zd != z) & (q == p))
        def _():
            fin_copy(z, zd).start()

        @pl.when((zd != z) & (q != p))
        def _():
            stg_copy(z, zd).start()

        return carry

    lax.fori_loop(0, n, pack, 0)

    for i in range(len(bits)):
        spread_round(0, i)
    give.wait_recv()
    spread_own(1)
    for i in range(len(bits)):
        spread_round(1, i)
    here.wait()
    for i in range(2):
        cot_copy(i).wait_recv()

    def forward(zs, src=None):
        src = stg.at[zs] if src is None else src
        return copy(src, fin.at[2 * zs + p], fwd_s.at[zs], fwd_r.at[zs], "fsdp", pair)

    def forward_state(j):
        zs = ring(length - j)
        stg_copy(zs, z).wait_recv()
        forward(zs).start()

    def state_here():
        for j in range(1, length):
            fin_copy(ring(j), z).wait_recv()
        for zs in range(length):
            got = fin.at[2 * zs + 1 - p]
            copy(stg.at[zs], got, fwd_s.at[zs], fwd_r.at[zs], "fsdp", pair).wait_recv()

    def term(d, k):
        def tile(i, carry):
            at = lanes(i, 2 * LANE)
            tmp[: sizes[k], at] = sum(
                jnp.dot(
                    at_buf[b, d, span(k), :], c_buf[b, :, at],
                    preferred_element_type=jnp.float32,
                )
                for b in range(2)
            )
            return carry

        lax.fori_loop(0, width // (2 * LANE), tile, 0)

    def send_up(k, s):
        slot = s - jnp.minimum(z, 1)
        return copy(
            up.at[slot, span(k)], up.at[s, span(k)], up_s.at[k, s], up_r.at[k, s], "fsdp", f + 2
        )

    def send_dn(k, s):
        slot = s - jnp.minimum(last - z, 1)
        return copy(
            dn.at[slot, span(k)], dn.at[s, span(k)], dn_s.at[k, s], dn_r.at[k, s], "fsdp", f - 2
        )

    def take_up(k, s):
        got = up.at[s, span(k)]
        copy(got, got, up_s.at[k, s], up_r.at[k, s], "fsdp", f - 2).wait_recv()

    def take_dn(k, s):
        got = dn.at[s, span(k)]
        copy(got, got, dn_s.at[k, s], dn_r.at[k, s], "fsdp", f + 2).wait_recv()

    def add_in(ref, k, slot, first):
        mine = pl.ds(0, sizes[k])

        @pl.when(first)
        def _():
            ref[slot, span(k), :] = tmp[mine, :].astype(jnp.bfloat16)

        @pl.when(jnp.logical_not(first))
        def _():
            total = tmp[mine, :] + ref[slot, span(k), :].astype(jnp.float32)
            ref[slot, span(k), :] = total.astype(jnp.bfloat16)

    def reduce_step(k, s):
        @pl.when(z <= s)
        def _():
            term(last + z - s, k)
            if s:

                @pl.when(z > 0)
                def _():
                    take_up(k, s - 1)

            add_in(up, k, s - jnp.minimum(z, 1), z == 0)
            send_up(k, s).start()

        @pl.when(z >= last - s)
        def _():
            term(s - last + z, k)
            if s:

                @pl.when(z < last)
                def _():
                    take_dn(k, s - 1)

            add_in(dn, k, s - jnp.minimum(last - z, 1), z == last)
            send_dn(k, s).start()

    sub = stage.shape[2]

    def out_copies(i, slot):
        return [
            pltpu.make_async_copy(stage.at[slot, a], dst.at[lanes(i, sub)], out_sem.at[slot, a])
            for a, dst in enumerate((w_out, m_out, v_out))
        ]

    def adam(k):
        term(z, k)
        if k == 0:
            state_here()

        def spin(i, carry):
            at = pl.ds(pl.multiple_of(starts[k] + i * LANE, LANE), LANE)
            for a in range(3):
                parts_of = [fin[src, a * cols : (a + 1) * cols, at] for src in range(n)]
                old[a, lanes(i, LANE), :] = jnp.concatenate(parts_of, axis=0).T
            return carry

        lax.fori_loop(0, sizes[k] // LANE, spin, 0)
        mine = pl.ds(0, sizes[k])

        @pl.when(z > 0)
        def _():
            take_up(k, last - 1)
            tmp[mine, :] += up[last - 1, span(k), :].astype(jnp.float32)

        @pl.when(z < last)
        def _():
            take_dn(k, last - 1)
            tmp[mine, :] += dn[last - 1, span(k), :].astype(jnp.float32)

        def piece(j, carry):
            i = starts[k] // sub + j
            slot = i % 2

            @pl.when(i >= 2)
            def _():
                for c in out_copies(i - 2, slot):
                    c.wait()

            at = lanes(j, sub)
            held_now = [old[a, at, :].astype(jnp.float32) for a in range(3)]
            new = adam_update(*held_now, tmp[at, :])
            for a in range(3):
                stage[slot, a] = new[a]
            wb[lanes(i, sub), :] = new[0].astype(jnp.bfloat16)
            for c in out_copies(i, slot):
                c.start()
            return carry

        lax.fori_loop(0, sizes[k] // sub, piece, 0)

    def block(c, q, k):
        return b_out.at[pl.ds(pl.multiple_of((2 * c + q) * rows + starts[k], LANE), sizes[k])]

    def to_pair(k, c, src=None):
        src = block(c, p, k) if src is None else src
        return copy(src, block(c, p, k), y_send.at[k, c], y_recv.at[k, c], "fsdp", pair)

    def to_right(k, s, src=None):
        src = block(z - s, p, k) if src is None else src
        return copy(src, block(z - s, p, k), r_send.at[k, s], r_recv.at[k, s], "fsdp", f + 2)

    def to_left(k, s, src=None):
        src = block(z + s, p, k) if src is None else src
        return copy(src, block(z + s, p, k), l_send.at[k, s], l_recv.at[k, s], "fsdp", f - 2)

    def keep(k):
        return pltpu.make_async_copy(wb.at[span(k)], block(z, p, k), own_sem.at[k])

    def gather_start(k):
        mine = wb.at[span(k)]
        to_pair(k, z, mine).start()

        @pl.when(z < last)
        def _():
            to_right(k, 0, mine).start()

        @pl.when(z > 0)
        def _():
            to_left(k, 0, mine).start()

        keep(k).start()

    def gather_step(k, s):
        @pl.when(z > s)
        def _():
            c = z - 1 - s
            got = block(c, p, k)
            copy(got, got, r_send.at[k, s], r_recv.at[k, s], "fsdp", f - 2).wait_recv()
            if s + 1 < last:

                @pl.when(z < last)
                def _():
                    to_right(k, s + 1).start()

            to_pair(k, c).start()

        @pl.when(z < last - s)
        def _():
            c = z + 1 + s
            got = block(c, p, k)
            copy(got, got, l_send.at[k, s], l_recv.at[k, s], "fsdp", f + 2).wait_recv()
            if s + 1 < last:

                @pl.when(z > 0)
                def _():
                    to_left(k, s + 1).start()

            to_pair(k, c).start()

    forward(z, st_out.at[pair]).start()
    waiting = []
    for s in range(last):
        reduce_step(0, s)
        forward_state(s + 1)
    for k in range(1, len(sizes)):
        reduce_step(k, 0)
        adam(k - 1)
        gather_start(k - 1)
        for g in waiting:
            gather_step(*g)
        waiting = [(k - 1, s) for s in range(last)]
        for s in range(1, last):
            reduce_step(k, s)
            gather_step(*waiting.pop(0))
    adam(len(sizes) - 1)
    gather_start(len(sizes) - 1)
    for g in waiting + [(len(sizes) - 1, s) for s in range(last)]:
        gather_step(*g)

    give.wait_send()
    for i in range(2):
        cot_copy(i).wait_send()
        spread_done(i)
    pieces = rows // sub
    for j in (2, 1):
        for c in out_copies(pieces - j, (pieces - j) % 2):
            c.wait()
    for j in range(1, length):
        fin_copy(z, ring(j)).wait_send()
        stg_copy(z, ring(j)).wait_send()
    for zs in range(length):
        forward(zs).wait_send()
    for k in range(len(sizes)):
        keep(k).wait()
        for s in range(last):

            @pl.when(z <= s)
            def _():
                send_up(k, s).wait_send()

            @pl.when(z >= last - s)
            def _():
                send_dn(k, s).wait_send()

            @pl.when((z < last) & (z >= s))
            def _():
                to_right(k, s).wait_send()

            @pl.when((z > 0) & (last - z >= s))
            def _():
                to_left(k, s).wait_send()

        for c in range(length):
            to_pair(k, c).wait_send()
            theirs = block(c, 1 - p, k)
            copy(theirs, theirs, y_send.at[k, c], y_recv.at[k, c], "fsdp", pair).wait_recv()


def row_chunks(rows):
    tiles = rows // LANE
    counts = [2] * (tiles // 2) + [1] * (tiles % 2)
    return tuple(c * LANE for c in counts)


def fast_body(activations, cotangent, weights, first_moment, second_moment, *, n, parts):
    depth, cols = weights.shape
    tok, width = activations.shape
    rows = depth // n
    length = n // 2
    sizes = row_chunks(rows)
    chunks = len(sizes)
    sub = LANE // 2
    rounds = parts.bit_length() - 1
    dma = pltpu.SemaphoreType.DMA
    half, full = jnp.bfloat16, jnp.float32
    hops = max(length - 1, 1)
    row = jax.ShapeDtypeStruct((rows, width), full)
    anywhere = pl.BlockSpec(memory_space=pl.ANY)
    return tuple(
        pl.pallas_call(
            functools.partial(fsdp_kernel, n, parts, sizes),
            out_shape=(row, row, row, jax.ShapeDtypeStruct((depth, width), half)),
            in_specs=[anywhere] * 5,
            out_specs=(anywhere,) * 4,
            scratch_shapes=[
                pltpu.VMEM((2, tok, rows), half),
                pltpu.VMEM((rows, tok), half),
                pltpu.VMEM((2, parts, rows, tok), half),
                pltpu.VMEM((2, tok, width), half),
                pltpu.VMEM((2, 3, cols, rows), full),
                pltpu.VMEM((n, 3 * cols, rows), half),
                pltpu.VMEM((n, 3 * cols, rows), half),
                pltpu.VMEM((length, 3 * cols, rows), half),
                pltpu.VMEM((hops, rows, width), half),
                pltpu.VMEM((hops, rows, width), half),
                pltpu.VMEM((max(sizes), width), full),
                pltpu.VMEM((3, max(sizes), width), half),
                pltpu.VMEM((2, 3, sub, width), full),
                pltpu.VMEM((rows, width), half),
                dma((2,)), dma, dma((2, 3)), dma((2, 3)), dma((chunks,)),
                dma, dma, dma((2,)), dma((2,)),
                dma((2, rounds, parts)), dma((2, parts)),
            ]
            + [dma((length,))] * 6
            + [dma((chunks, hops))] * 4
            + [dma((chunks, length))] * 2
            + [dma((chunks, hops))] * 4,
            compiler_params=pltpu.CompilerParams(
                collective_id=0, has_side_effects=True, vmem_limit_bytes=67043328
            ),
            name="fsdp_step",
        )(activations, cotangent, weights.T, first_moment.T, second_moment.T)
    )


def solution(mesh):
    n, parts = mesh.shape["fsdp"], mesh.shape["tensor"]

    def run(*arrays):
        rows, width = arrays[2].shape[0] // n, arrays[0].shape[1]
        fits = rows % LANE == 0 and n == 2 * parts and width == 2 * rows
        if fits and arrays[2].shape[1] % 16 == 0 and parts & (parts - 1) == 0:
            return fast_body(*arrays, n=n, parts=parts)
        return body(*arrays, n=n, parts=parts)

    return jax.shard_map(
        run,
        mesh=mesh,
        in_specs=(
            P("fsdp", "tensor"),
            P("fsdp", "tensor"),
            P(None, ("tensor", "fsdp")),
            P(None, ("tensor", "fsdp")),
            P(None, ("tensor", "fsdp")),
        ),
        out_specs=(
            P("fsdp", "tensor"),
            P("fsdp", "tensor"),
            P("fsdp", "tensor"),
            P(None, "tensor"),
        ),
        check_vma=False,
    )
```

```python
import functools

import jax
import jax.numpy as jnp
from jax import lax
from jax.experimental import pallas as pl
from jax.experimental.pallas import tpu as pltpu
from jax.sharding import PartitionSpec as P


STEP = 20


beta_one = 0.9
beta_two = 0.95
adam_eps = 1e-08
learn_rate = 0.0003
decay_rate = 0.1


def adam_update(weights, first_moment, second_moment, gradient):
    first_new = beta_one * first_moment + (1.0 - beta_one) * gradient
    second_new = beta_two * second_moment + (1.0 - beta_two) * gradient * gradient
    corrected = first_new / (1.0 - beta_one**STEP)
    scaled = jnp.sqrt(second_new / (1.0 - beta_two**STEP)) + adam_eps
    weights_new = weights - learn_rate * (corrected / scaled + decay_rate * weights)
    return (weights_new, first_new, second_new)


def line_pairs(length, step, senders):
    return [
        (2 * z + p, 2 * (z + step) + p)
        for z in range(length)
        for p in range(2)
        if senders(z) and 0 <= z + step < length
    ]


def reduce_line(term, z, length):
    last = length - 1
    right = left = None
    for s in range(last):
        up = term(jnp.clip(last + z - s, 0, last))
        down = term(jnp.clip(s - last + z, 0, last))
        if s:
            up = (up.astype(jnp.float32) + right.astype(jnp.float32)).astype(jnp.bfloat16)
            down = (down.astype(jnp.float32) + left.astype(jnp.float32)).astype(jnp.bfloat16)
        right = lax.ppermute(up, "fsdp", line_pairs(length, 1, lambda i: i <= s))
        left = lax.ppermute(down, "fsdp", line_pairs(length, -1, lambda i: i >= last - s))
    own = term(z)
    own = own.astype(jnp.float32)
    if last:
        own = own + right.astype(jnp.float32) + left.astype(jnp.float32)
    return own


def gather_kernel(
    length, own_ref, out_ref, local_sem, y_send, y_recv, r_send, r_recv, l_send, l_recv
):
    f = lax.axis_index("fsdp")
    z, p = f // 2, f % 2
    last = length - 1
    rows = own_ref.shape[0]
    pair, right, left = f + 1 - 2 * p, f + 2, f - 2

    def block(c):
        return out_ref.at[pl.ds((2 * c + p) * rows, rows)]

    def copy(src, dst, send, recv, target):
        return pltpu.make_async_remote_copy(
            src_ref=src,
            dst_ref=dst,
            send_sem=send,
            recv_sem=recv,
            device_id={"fsdp": target},
            device_id_type=pl.DeviceIdType.MESH,
        )

    def to_pair(c, src=None):
        return copy(block(c) if src is None else src, block(c), y_send.at[c], y_recv.at[c], pair)

    def to_right(s, src=None):
        c = z - s
        return copy(block(c) if src is None else src, block(c), r_send.at[s], r_recv.at[s], right)

    def to_left(s, src=None):
        c = z + s
        return copy(block(c) if src is None else src, block(c), l_send.at[s], l_recv.at[s], left)

    barrier = pltpu.get_barrier_semaphore()
    pl.semaphore_signal(
        barrier, inc=1, device_id={"fsdp": pair}, device_id_type=pl.DeviceIdType.MESH
    )

    @pl.when(z > 0)
    def _():
        pl.semaphore_signal(
            barrier, inc=1, device_id={"fsdp": left}, device_id_type=pl.DeviceIdType.MESH
        )

    @pl.when(z < last)
    def _():
        pl.semaphore_signal(
            barrier, inc=1, device_id={"fsdp": right}, device_id_type=pl.DeviceIdType.MESH
        )

    span = max(last, 1)
    pl.semaphore_wait(barrier, 1 + (z + span - 1) // span + (last - z + span - 1) // span)

    @pl.when(z < last)
    def _():
        to_right(0, own_ref).start()

    @pl.when(z > 0)
    def _():
        to_left(0, own_ref).start()

    to_pair(z, own_ref).start()
    here = pltpu.make_async_copy(own_ref, block(z), local_sem)
    here.start()

    for s in range(last):

        @pl.when(z > s)
        def _():
            c = z - 1 - s
            copy(block(c), block(c), r_send.at[s], r_recv.at[s], left).wait_recv()
            if s + 1 < last:

                @pl.when(z < last)
                def _():
                    to_right(s + 1).start()

            to_pair(c).start()

        @pl.when(z < last - s)
        def _():
            c = z + 1 + s
            copy(block(c), block(c), l_send.at[s], l_recv.at[s], right).wait_recv()
            if s + 1 < last:

                @pl.when(z > 0)
                def _():
                    to_left(s + 1).start()

            to_pair(c).start()

    for s in range(last):

        @pl.when((z < last) & (z >= s))
        def _():
            to_right(s).wait_send()

        @pl.when((z > 0) & (last - z >= s))
        def _():
            to_left(s).wait_send()

    here.wait()
    for c in range(length):
        to_pair(c).wait_send()
        theirs = out_ref.at[pl.ds((2 * c + 1 - p) * rows, rows)]
        copy(theirs, theirs, y_send.at[c], y_recv.at[c], pair).wait_recv()


def gather_line(own, length):
    rows, cols = own.shape
    dma = pltpu.SemaphoreType.DMA
    steps = max(length - 1, 1)
    return pl.pallas_call(
        functools.partial(gather_kernel, length),
        out_shape=jax.ShapeDtypeStruct((2 * length * rows, cols), own.dtype),
        in_specs=[pl.BlockSpec(memory_space=pltpu.VMEM)],
        out_specs=pl.BlockSpec(memory_space=pl.ANY),
        scratch_shapes=[dma, dma((length,)), dma((length,))] + [dma((steps,))] * 4,
        compiler_params=pltpu.CompilerParams(collective_id=0, has_side_effects=True),
        name="gather_rows",
    )(own)


def body(activations, cotangent, weights, first_moment, second_moment, *, n, parts):
    f = lax.axis_index("fsdp")
    z, p = f // 2, f % 2
    length = n // 2
    depth, cols = weights.shape
    rows = depth // n
    tok, width = activations.shape
    pair = [(i, i ^ 1) for i in range(n)]

    packed = jnp.concatenate([weights, first_moment, second_moment], axis=1).astype(jnp.bfloat16)
    lines = [[2 * i + q for i in range(length)] for q in range(2)]
    packed = lax.optimization_barrier(packed.reshape(length, 2, rows, 3 * cols))
    along = lax.all_to_all(packed, "fsdp", 0, 0, axis_index_groups=lines)
    blocks = activations.reshape(tok, width // (2 * rows), 2, rows)
    keep = lax.dynamic_index_in_dim(blocks, p, 2, False).reshape(tok, width // 2)
    give = lax.dynamic_index_in_dim(blocks, 1 - p, 2, False).reshape(tok, width // 2)
    got = lax.ppermute(give, "fsdp", pair)
    cot_peer = lax.ppermute(cotangent, "fsdp", pair)
    mine = lax.all_gather(keep, "tensor")
    theirs = lax.all_gather(got, "tensor")

    def product(a, b):
        return lax.dot_general(a, b, (((0,), (0,)), ((), ())), preferred_element_type=jnp.float32)

    groups = length // parts

    def term(c):
        at = (c // groups, 0, (c % groups) * rows)
        near, far = (
            lax.dynamic_slice(array, at, (1, tok, rows))[0] for array in (mine, theirs)
        )
        total = product(near, cotangent) + product(far, cot_peer)
        return lax.optimization_barrier(total.astype(jnp.bfloat16))

    gradient = reduce_line(term, z, length)

    stay = lax.dynamic_index_in_dim(along, p, 1, False)
    across = lax.ppermute(lax.dynamic_index_in_dim(along, 1 - p, 1, False), "fsdp", pair)
    moved = jnp.where(p == 0, jnp.stack([stay, across], 1), jnp.stack([across, stay], 1))

    def owned(k):
        pieces = [moved[i // 2, i % 2, :, k * cols : (k + 1) * cols] for i in range(n)]
        return lax.optimization_barrier(jnp.concatenate(pieces, axis=1)).astype(jnp.float32)

    weights_new, first_new, second_new = adam_update(owned(0), owned(1), owned(2), gradient)
    rounded = weights_new.astype(jnp.bfloat16)
    weights_bf16 = gather_line(rounded, length)
    return (weights_new, first_new, second_new, weights_bf16)


LANE = 128


def fsdp_kernel(
    n, parts, sizes, batches, relays, order, act, cot, w_in, m_in, v_in, w_out, m_out, v_out, b_out,
    raw, give_t, at_buf, c_buf, st_in, st_out, fin, stg, up, dn, tmp, old, wb,
    raw_sem, loc_sem, st_sem, own_sem, give_s, give_r, cot_s, cot_r,
    t_send, t_recv, fin_s, fin_r, stg_s, stg_r, fwd_s, fwd_r,
    up_s, up_r, dn_s, dn_r, y_send, y_recv, r_send, r_recv, l_send, l_recv, x_send, x_recv,
):
    f = lax.axis_index("fsdp")
    t = lax.axis_index("tensor")
    z, p = f // 2, f % 2
    length = n // 2
    last = length - 1
    tok, width = act.shape
    rows, cols = at_buf.shape[2], w_in.shape[0]
    pair = f + 1 - 2 * p
    bits = [1 << i for i in range(parts.bit_length() - 1)][::-1]
    starts = [sum(sizes[:k]) for k in range(len(sizes))]

    def copy(src, dst, send, recv, axis, target):
        return pltpu.make_async_remote_copy(
            src_ref=src, dst_ref=dst, send_sem=send, recv_sem=recv,
            device_id={axis: target}, device_id_type=pl.DeviceIdType.MESH,
        )

    def crossed(i, b):
        return i + b - 2 * b * ((t // b) % 2)

    def ring(j):
        return (z + j) % length

    def span(k):
        return pl.ds(starts[k], sizes[k])

    def lanes(i, size):
        return pl.ds(pl.multiple_of(i * size, size), size)

    def feature(q):
        return lanes(q, rows)

    raw_copies = [
        pltpu.make_async_copy(act.at[:, feature(q)], raw.at[i], raw_sem.at[i])
        for i, q in enumerate((1 - p, p))
    ]
    for c in raw_copies:
        c.start()
    here = pltpu.make_async_copy(cot, c_buf.at[0], loc_sem)
    here.start()

    firsts = [sum(batches[:i]) for i in range(len(batches))]

    def batch(i):
        return pl.ds(firsts[i], batches[i])

    def load_state(i, u, slot):
        d = 2 * ring(u + 1) + (p + 1 + u // length) % 2
        at = pl.ds(pl.multiple_of(d * rows + firsts[i], LANE), batches[i])
        return [
            pltpu.make_async_copy(
                src.at[:, at], st_in.at[slot, a, :, pl.ds(0, batches[i])], st_sem.at[slot, a]
            )
            for a, src in enumerate((w_in, m_in, v_in))
        ]

    for c in load_state(0, 0, 0):
        c.start()

    barrier = pltpu.get_barrier_semaphore()

    def greet(axis, target):
        pl.semaphore_signal(
            barrier, inc=1, device_id={axis: target}, device_id_type=pl.DeviceIdType.MESH
        )

    greet("fsdp", pair)
    for j in range(1, length):
        greet("fsdp", 2 * ring(j) + p)
    for b in bits:
        greet("tensor", crossed(t, b))
    pl.semaphore_wait(barrier, length + len(bits))

    head = tok // 4

    def cot_copy(i):
        at = pl.ds(0, head) if i == 0 else pl.ds(head, tok - head)
        return copy(cot.at[at], c_buf.at[1, at], cot_s.at[i], cot_r.at[i], "fsdp", pair)

    def turn(src, dst):
        def tile(r, carry):
            dst[lanes(r, LANE), :] = src[:, lanes(r, LANE)].T
            return carry

        lax.fori_loop(0, rows // LANE, tile, 0)

    def block_copy(which, i, h):
        return copy(
            at_buf.at[which, h], at_buf.at[which, h], t_send.at[which, i, h],
            t_recv.at[which, h], "tensor", crossed(t, bits[i]),
        )

    def held(i):
        found = [t]
        for b in bits[:i]:
            found = found + [crossed(h, b) for h in found]
        return found

    def spread_own(which):
        for i in range(len(bits)):
            block_copy(which, i, t).start()

    def spread_round(which, i):
        for h in held(i):
            g = crossed(h, bits[i])
            block_copy(which, i, g).wait_recv()
            for j in range(i + 1, len(bits)):
                block_copy(which, j, g).start()

    def spread_done(which):
        for i in range(len(bits)):
            for h in held(i):
                block_copy(which, i, h).wait_send()

    def fin_copy(i, zs, zd):
        return copy(
            st_out.at[2 * zd + p, :, batch(i)], fin.at[2 * zs + p, :, batch(i)],
            fin_s.at[i, zd], fin_r.at[i, zs], "fsdp", 2 * zd + p,
        )

    def stg_copy(i, zs, zd):
        return copy(
            st_out.at[2 * zd + 1 - p, :, batch(i)], stg.at[zs, :, batch(i)],
            stg_s.at[i, zd], stg_r.at[i, zs], "fsdp", 2 * zd + p,
        )

    def pack(i, u, carry):
        slot = u % 2

        @pl.when(u + 1 < n)
        def _():
            for c in load_state(i, u + 1, (u + 1) % 2):
                c.start()

        for c in load_state(i, u, slot):
            c.wait()
        zd, q = ring(u + 1), (p + 1 + u // length) % 2
        d = 2 * zd + q
        for a in range(3):
            st_out[d, a * cols : (a + 1) * cols, batch(i)] = st_in[
                slot, a, :, : batches[i]
            ].astype(jnp.bfloat16)

        @pl.when(d == f)
        def _():
            fin[d, :, batch(i)] = st_out[d, :, batch(i)]

        @pl.when((zd != z) & (q == p))
        def _():
            fin_copy(i, z, zd).start()

        @pl.when((zd != z) & (q != p))
        def _():
            stg_copy(i, z, zd).start()

        return carry

    cot_copy(0).start()
    for i in range(len(batches)):
        if i:
            for c in load_state(i, 0, 0):
                c.start()
        lax.fori_loop(0, n, functools.partial(pack, i), 0)

    raw_copies[0].wait()
    turn(raw.at[0], give_t)
    give = copy(give_t, at_buf.at[1, t], give_s, give_r, "fsdp", pair)
    give.start()
    cot_copy(1).start()
    raw_copies[1].wait()
    turn(raw.at[1], at_buf.at[0, t])
    spread_own(0)

    for i in range(len(bits)):
        spread_round(0, i)
    give.wait_recv()
    spread_own(1)
    for i in range(len(bits)):
        spread_round(1, i)
    here.wait()
    for i in range(2):
        cot_copy(i).wait_recv()

    def forward(i, zs, src=None):
        src = stg.at[zs, :, batch(i)] if src is None else src
        return copy(
            src, fin.at[2 * zs + p, :, batch(i)], fwd_s.at[i, zs], fwd_r.at[i, zs], "fsdp", pair
        )

    def forward_state(j, i):
        if j:
            zs = ring(length - j)
            stg_copy(i, zs, z).wait_recv()
            forward(i, zs).start()
        else:
            forward(i, z, st_out.at[pair, :, batch(i)]).start()

    def state_here(i):
        for j in range(1, length):
            fin_copy(i, ring(j), z).wait_recv()
        for zs in range(length):
            got = fin.at[2 * zs + 1 - p, :, batch(i)]
            forward_here = copy(got, got, fwd_s.at[i, zs], fwd_r.at[i, zs], "fsdp", pair)
            forward_here.wait_recv()

    def term(d, k):
        def tile(i, carry):
            at = lanes(i, width // 2)
            tmp[: sizes[k], at] = sum(
                jnp.dot(
                    at_buf[b, d, span(k), :], c_buf[b, :, at],
                    preferred_element_type=jnp.float32,
                )
                for b in range(2)
            )
            return carry

        lax.fori_loop(0, 2, tile, 0)

    def send_up(k, s):
        slot = s - jnp.minimum(z, 1)
        return copy(
            up.at[slot, span(k)], up.at[s, span(k)], up_s.at[k, s], up_r.at[k, s], "fsdp", f + 2
        )

    def send_dn(k, s):
        slot = s - jnp.minimum(last - z, 1)
        return copy(
            dn.at[slot, span(k)], dn.at[s, span(k)], dn_s.at[k, s], dn_r.at[k, s], "fsdp", f - 2
        )

    def take_up(k, s):
        got = up.at[s, span(k)]
        copy(got, got, up_s.at[k, s], up_r.at[k, s], "fsdp", f - 2).wait_recv()

    def take_dn(k, s):
        got = dn.at[s, span(k)]
        copy(got, got, dn_s.at[k, s], dn_r.at[k, s], "fsdp", f + 2).wait_recv()

    def add_in(ref, k, slot, first):
        mine = pl.ds(0, sizes[k])

        @pl.when(first)
        def _():
            ref[slot, span(k), :] = tmp[mine, :].astype(jnp.bfloat16)

        @pl.when(jnp.logical_not(first))
        def _():
            total = tmp[mine, :] + ref[slot, span(k), :].astype(jnp.float32)
            ref[slot, span(k), :] = total.astype(jnp.bfloat16)

    def reduce_step(k, s):
        @pl.when(z <= s)
        def _():
            term(last + z - s, k)
            if s:

                @pl.when(z > 0)
                def _():
                    take_up(k, s - 1)

            add_in(up, k, s - jnp.minimum(z, 1), z == 0)
            send_up(k, s).start()

        @pl.when(z >= last - s)
        def _():
            term(s - last + z, k)
            if s:

                @pl.when(z < last)
                def _():
                    take_dn(k, s - 1)

            add_in(dn, k, s - jnp.minimum(last - z, 1), z == last)
            send_dn(k, s).start()

    sub = LANE // 2

    arrived = []

    def adam(k):
        term(z, k)
        for i in range(len(batches)):
            if i not in arrived and firsts[i] < starts[k] + sizes[k]:
                state_here(i)
                arrived.append(i)

        def spin(i, carry):
            at = pl.ds(pl.multiple_of(starts[k] + i * LANE, LANE), LANE)
            for a in range(3):
                parts_of = [fin[src, a * cols : (a + 1) * cols, at] for src in range(n)]
                old[a, lanes(i, LANE), :] = jnp.concatenate(parts_of, axis=0).T
            return carry

        lax.fori_loop(0, sizes[k] // LANE, spin, 0)
        mine = pl.ds(0, sizes[k])

        @pl.when(z > 0)
        def _():
            take_up(k, last - 1)
            tmp[mine, :] += up[last - 1, span(k), :].astype(jnp.float32)

        @pl.when(z < last)
        def _():
            take_dn(k, last - 1)
            tmp[mine, :] += dn[last - 1, span(k), :].astype(jnp.float32)

        def piece(j, carry):
            to = lanes(starts[k] // sub + j, sub)
            at = lanes(j, sub)
            held_now = [old[a, at, :].astype(jnp.float32) for a in range(3)]
            new = adam_update(*held_now, tmp[at, :])
            for a, out in enumerate((w_out, m_out, v_out)):
                out[to, :] = new[a]
            wb[to, :] = new[0].astype(jnp.bfloat16)
            return carry

        lax.fori_loop(0, sizes[k] // sub, piece, 0)
        gather_start(k)

    def block(c, q, k):
        return b_out.at[pl.ds(pl.multiple_of((2 * c + q) * rows + starts[k], LANE), sizes[k])]

    def to_pair(k, c, src=None):
        src = block(c, p, k) if src is None else src
        return copy(src, block(c, p, k), y_send.at[k, c], y_recv.at[k, c], "fsdp", pair)

    def to_right(k, s, src=None):
        src = block(z - s, p, k) if src is None else src
        return copy(src, block(z - s, p, k), r_send.at[k, s], r_recv.at[k, s], "fsdp", f + 2)

    def to_left(k, s, src=None):
        src = block(z + s, p, k) if src is None else src
        return copy(src, block(z + s, p, k), l_send.at[k, s], l_recv.at[k, s], "fsdp", f - 2)

    def keep(k):
        return pltpu.make_async_copy(wb.at[span(k)], block(z, p, k), own_sem.at[k])

    def gather_start(k):
        mine = wb.at[span(k)]
        to_pair(k, z, mine).start()

        @pl.when(z < last)
        def _():
            to_right(k, 0, mine).start()

        @pl.when(z > 0)
        def _():
            to_left(k, 0, mine).start()

        keep(k).start()

    even = z % 2 == 0
    beside = z + 1 - 2 * (z % 2)

    def relay(k):
        got = block(z, 1 - p, k)
        copy(got, got, y_send.at[k, z], y_recv.at[k, z], "fsdp", pair).wait_recv()
        relay_copy(k, z).start()

    def relay_copy(k, c):
        got = block(c, 1 - p, k)
        return copy(got, got, x_send.at[k], x_recv.at[k], "fsdp", 2 * beside + p)

    def onward(k, s, c, near):
        if s or k not in relays:
            to_pair(k, c).start()
        else:

            @pl.when(jnp.logical_not(near))
            def _():
                to_pair(k, c).start()

    def gather_step(k, s):
        @pl.when(z > s)
        def _():
            c = z - 1 - s
            got = block(c, p, k)
            copy(got, got, r_send.at[k, s], r_recv.at[k, s], "fsdp", f - 2).wait_recv()
            if s + 1 < last:

                @pl.when(z < last)
                def _():
                    to_right(k, s + 1).start()

            onward(k, s, c, z % 2 == 1)

        @pl.when(z < last - s)
        def _():
            c = z + 1 + s
            got = block(c, p, k)
            copy(got, got, l_send.at[k, s], l_recv.at[k, s], "fsdp", f + 2).wait_recv()
            if s + 1 < last:

                @pl.when(z > 0)
                def _():
                    to_left(k, s + 1).start()

            onward(k, s, c, even)


    forward_state(0, 0)
    for kind, *at in order:
        {
            "F": forward_state, "R": reduce_step, "A": adam, "G": gather_step, "X": relay,
        }[kind](*at)

    give.wait_send()
    for i in range(2):
        cot_copy(i).wait_send()
        spread_done(i)
    for i in range(len(batches)):
        for j in range(1, length):
            fin_copy(i, z, ring(j)).wait_send()
            stg_copy(i, z, ring(j)).wait_send()
        for zs in range(length):
            forward(i, zs).wait_send()
    for k in range(len(sizes)):
        keep(k).wait()
        for s in range(last):

            @pl.when(z <= s)
            def _():
                send_up(k, s).wait_send()

            @pl.when(z >= last - s)
            def _():
                send_dn(k, s).wait_send()

            @pl.when((z < last) & (z >= s))
            def _():
                to_right(k, s).wait_send()

            @pl.when((z > 0) & (last - z >= s))
            def _():
                to_left(k, s).wait_send()

        if k in relays:
            relay_copy(k, z).wait_send()
            relay_copy(k, beside).wait_recv()
            to_pair(k, z).wait_send()
            others = [ring(j) for j in range(1, length)]
        else:
            others = list(range(length))

        def settle(c):
            to_pair(k, c).wait_send()
            theirs = block(c, 1 - p, k)
            copy(theirs, theirs, y_send.at[k, c], y_recv.at[k, c], "fsdp", pair).wait_recv()

        for c in others:
            if k in relays:
                pl.when(c != beside)(functools.partial(settle, c))
            else:
                settle(c)


TUNED = (
    "F01 R00 F30 R01",
    "F10 F20 R10 F31",
    "R02 F11 R20 A0",
    "R11 F21 G00 R12",
    "R30 G01 R21 A1",
    "G02 R22 R40 G10",
    "R31 A2 G11 R32",
    "G20 G12 R41 A3",
    "G21 R42 G30 G22",
    "A4 G31 G40 G32",
    "G41 X0 G42 X1",
)
RELAYS = (0, 1)
FIRST_BATCH = 1


def step_order(chunks, last):
    if (chunks, last) == (5, 3):
        order = [(w[0], *(int(c) for c in w[1:])) for w in " ".join(TUNED).split()]
        first = FIRST_BATCH
        return tuple(order), RELAYS, (first, chunks - first) if first < chunks else (chunks,)
    order = [("F", j + 1, 0) for j in range(last)]
    for k in range(chunks):
        order += [("R", k, s) for s in range(last)] + [("A", k)]
        order += [("G", k, s) for s in range(last)]
    return tuple(order), (), (chunks,)


def fast_body(activations, cotangent, weights, first_moment, second_moment, *, n, parts):
    depth, cols = weights.shape
    tok, width = activations.shape
    rows = depth // n
    length = n // 2
    sizes = (LANE,) * (rows // LANE)
    chunks = len(sizes)
    order, relays, batches = step_order(chunks, length - 1)
    batches = tuple(b * LANE for b in batches)
    rounds = parts.bit_length() - 1
    dma = pltpu.SemaphoreType.DMA
    half, full = jnp.bfloat16, jnp.float32
    hops = max(length - 1, 1)
    row = pltpu.VMEM((rows, width), full)
    anywhere = pl.BlockSpec(memory_space=pl.ANY)
    return tuple(
        pl.pallas_call(
            functools.partial(fsdp_kernel, n, parts, sizes, batches, relays, order),
            out_shape=(row, row, row, jax.ShapeDtypeStruct((depth, width), half)),
            in_specs=[anywhere] * 5,
            out_specs=(pl.BlockSpec(memory_space=pltpu.VMEM),) * 3 + (anywhere,),
            scratch_shapes=[
                pltpu.VMEM((2, tok, rows), half),
                pltpu.VMEM((rows, tok), half),
                pltpu.VMEM((2, parts, rows, tok), half),
                pltpu.VMEM((2, tok, width), half),
                pltpu.VMEM((2, 3, cols, rows), full),
                pltpu.VMEM((n, 3 * cols, rows), half),
                pltpu.VMEM((n, 3 * cols, rows), half),
                pltpu.VMEM((length, 3 * cols, rows), half),
                pltpu.VMEM((hops, rows, width), half),
                pltpu.VMEM((hops, rows, width), half),
                pltpu.VMEM((max(sizes), width), full),
                pltpu.VMEM((3, max(sizes), width), half),
                pltpu.VMEM((rows, width), half),
                dma((2,)), dma, dma((2, 3)), dma((chunks,)),
                dma, dma, dma((2,)), dma((2,)),
                dma((2, rounds, parts)), dma((2, parts)),
            ]
            + [dma((len(batches), length))] * 6
            + [dma((chunks, hops))] * 4
            + [dma((chunks, length))] * 2
            + [dma((chunks, hops))] * 4
            + [dma((chunks,))] * 2,
            compiler_params=pltpu.CompilerParams(
                collective_id=0, has_side_effects=True, vmem_limit_bytes=54 * 2**20
            ),
            name="fsdp_step",
        )(activations, cotangent, weights.T, first_moment.T, second_moment.T)
    )


def solution(mesh):
    n, parts = mesh.shape["fsdp"], mesh.shape["tensor"]

    def run(*arrays):
        rows, width = arrays[2].shape[0] // n, arrays[0].shape[1]
        fits = rows % LANE == 0 and n == 2 * parts and width == 2 * rows
        if fits and arrays[2].shape[1] % 16 == 0 and parts & (parts - 1) == 0:
            return fast_body(*arrays, n=n, parts=parts)
        return body(*arrays, n=n, parts=parts)

    return jax.shard_map(
        run,
        mesh=mesh,
        in_specs=(
            P("fsdp", "tensor"),
            P("fsdp", "tensor"),
            P(None, ("tensor", "fsdp")),
            P(None, ("tensor", "fsdp")),
            P(None, ("tensor", "fsdp")),
        ),
        out_specs=(
            P("fsdp", "tensor"),
            P("fsdp", "tensor"),
            P("fsdp", "tensor"),
            P(None, "tensor"),
        ),
        check_vma=False,
    )
```

```python
import functools

import jax
import jax.numpy as jnp
from jax import lax
from jax.experimental import pallas as pl
from jax.experimental.pallas import tpu as pltpu
from jax.sharding import PartitionSpec as P


STEP = 20


beta_one = 0.9
beta_two = 0.95
adam_eps = 1e-08
learn_rate = 0.0003
decay_rate = 0.1


def adam_update(weights, first_moment, second_moment, gradient):
    first_new = beta_one * first_moment + (1.0 - beta_one) * gradient
    second_new = beta_two * second_moment + (1.0 - beta_two) * gradient * gradient
    corrected = first_new / (1.0 - beta_one**STEP)
    scaled = jnp.sqrt(second_new / (1.0 - beta_two**STEP)) + adam_eps
    weights_new = weights - learn_rate * (corrected / scaled + decay_rate * weights)
    return (weights_new, first_new, second_new)


def line_pairs(length, step, senders):
    return [
        (2 * z + p, 2 * (z + step) + p)
        for z in range(length)
        for p in range(2)
        if senders(z) and 0 <= z + step < length
    ]


def reduce_line(term, z, length):
    last = length - 1
    right = left = None
    for s in range(last):
        up = term(jnp.clip(last + z - s, 0, last))
        down = term(jnp.clip(s - last + z, 0, last))
        if s:
            up = (up.astype(jnp.float32) + right.astype(jnp.float32)).astype(jnp.bfloat16)
            down = (down.astype(jnp.float32) + left.astype(jnp.float32)).astype(jnp.bfloat16)
        right = lax.ppermute(up, "fsdp", line_pairs(length, 1, lambda i: i <= s))
        left = lax.ppermute(down, "fsdp", line_pairs(length, -1, lambda i: i >= last - s))
    own = term(z)
    own = own.astype(jnp.float32)
    if last:
        own = own + right.astype(jnp.float32) + left.astype(jnp.float32)
    return own


def gather_kernel(
    length, own_ref, out_ref, local_sem, y_send, y_recv, r_send, r_recv, l_send, l_recv
):
    f = lax.axis_index("fsdp")
    z, p = f // 2, f % 2
    last = length - 1
    rows = own_ref.shape[0]
    pair, right, left = f + 1 - 2 * p, f + 2, f - 2

    def block(c):
        return out_ref.at[pl.ds((2 * c + p) * rows, rows)]

    def copy(src, dst, send, recv, target):
        return pltpu.make_async_remote_copy(
            src_ref=src,
            dst_ref=dst,
            send_sem=send,
            recv_sem=recv,
            device_id={"fsdp": target},
            device_id_type=pl.DeviceIdType.MESH,
        )

    def to_pair(c, src=None):
        return copy(block(c) if src is None else src, block(c), y_send.at[c], y_recv.at[c], pair)

    def to_right(s, src=None):
        c = z - s
        return copy(block(c) if src is None else src, block(c), r_send.at[s], r_recv.at[s], right)

    def to_left(s, src=None):
        c = z + s
        return copy(block(c) if src is None else src, block(c), l_send.at[s], l_recv.at[s], left)

    barrier = pltpu.get_barrier_semaphore()
    pl.semaphore_signal(
        barrier, inc=1, device_id={"fsdp": pair}, device_id_type=pl.DeviceIdType.MESH
    )

    @pl.when(z > 0)
    def _():
        pl.semaphore_signal(
            barrier, inc=1, device_id={"fsdp": left}, device_id_type=pl.DeviceIdType.MESH
        )

    @pl.when(z < last)
    def _():
        pl.semaphore_signal(
            barrier, inc=1, device_id={"fsdp": right}, device_id_type=pl.DeviceIdType.MESH
        )

    span = max(last, 1)
    pl.semaphore_wait(barrier, 1 + (z + span - 1) // span + (last - z + span - 1) // span)

    @pl.when(z < last)
    def _():
        to_right(0, own_ref).start()

    @pl.when(z > 0)
    def _():
        to_left(0, own_ref).start()

    to_pair(z, own_ref).start()
    here = pltpu.make_async_copy(own_ref, block(z), local_sem)
    here.start()

    for s in range(last):

        @pl.when(z > s)
        def _():
            c = z - 1 - s
            copy(block(c), block(c), r_send.at[s], r_recv.at[s], left).wait_recv()
            if s + 1 < last:

                @pl.when(z < last)
                def _():
                    to_right(s + 1).start()

            to_pair(c).start()

        @pl.when(z < last - s)
        def _():
            c = z + 1 + s
            copy(block(c), block(c), l_send.at[s], l_recv.at[s], right).wait_recv()
            if s + 1 < last:

                @pl.when(z > 0)
                def _():
                    to_left(s + 1).start()

            to_pair(c).start()

    for s in range(last):

        @pl.when((z < last) & (z >= s))
        def _():
            to_right(s).wait_send()

        @pl.when((z > 0) & (last - z >= s))
        def _():
            to_left(s).wait_send()

    here.wait()
    for c in range(length):
        to_pair(c).wait_send()
        theirs = out_ref.at[pl.ds((2 * c + 1 - p) * rows, rows)]
        copy(theirs, theirs, y_send.at[c], y_recv.at[c], pair).wait_recv()


def gather_line(own, length):
    rows, cols = own.shape
    dma = pltpu.SemaphoreType.DMA
    steps = max(length - 1, 1)
    return pl.pallas_call(
        functools.partial(gather_kernel, length),
        out_shape=jax.ShapeDtypeStruct((2 * length * rows, cols), own.dtype),
        in_specs=[pl.BlockSpec(memory_space=pltpu.VMEM)],
        out_specs=pl.BlockSpec(memory_space=pl.ANY),
        scratch_shapes=[dma, dma((length,)), dma((length,))] + [dma((steps,))] * 4,
        compiler_params=pltpu.CompilerParams(collective_id=0, has_side_effects=True),
        name="gather_rows",
    )(own)


def body(activations, cotangent, weights, first_moment, second_moment, *, n, parts):
    f = lax.axis_index("fsdp")
    z, p = f // 2, f % 2
    length = n // 2
    depth, cols = weights.shape
    rows = depth // n
    tok, width = activations.shape
    pair = [(i, i ^ 1) for i in range(n)]

    packed = jnp.concatenate([weights, first_moment, second_moment], axis=1).astype(jnp.bfloat16)
    lines = [[2 * i + q for i in range(length)] for q in range(2)]
    packed = lax.optimization_barrier(packed.reshape(length, 2, rows, 3 * cols))
    along = lax.all_to_all(packed, "fsdp", 0, 0, axis_index_groups=lines)
    blocks = activations.reshape(tok, width // (2 * rows), 2, rows)
    keep = lax.dynamic_index_in_dim(blocks, p, 2, False).reshape(tok, width // 2)
    give = lax.dynamic_index_in_dim(blocks, 1 - p, 2, False).reshape(tok, width // 2)
    got = lax.ppermute(give, "fsdp", pair)
    cot_peer = lax.ppermute(cotangent, "fsdp", pair)
    mine = lax.all_gather(keep, "tensor")
    theirs = lax.all_gather(got, "tensor")

    def product(a, b):
        return lax.dot_general(a, b, (((0,), (0,)), ((), ())), preferred_element_type=jnp.float32)

    groups = length // parts

    def term(c):
        at = (c // groups, 0, (c % groups) * rows)
        near, far = (
            lax.dynamic_slice(array, at, (1, tok, rows))[0] for array in (mine, theirs)
        )
        total = product(near, cotangent) + product(far, cot_peer)
        return lax.optimization_barrier(total.astype(jnp.bfloat16))

    gradient = reduce_line(term, z, length)

    stay = lax.dynamic_index_in_dim(along, p, 1, False)
    across = lax.ppermute(lax.dynamic_index_in_dim(along, 1 - p, 1, False), "fsdp", pair)
    moved = jnp.where(p == 0, jnp.stack([stay, across], 1), jnp.stack([across, stay], 1))

    def owned(k):
        pieces = [moved[i // 2, i % 2, :, k * cols : (k + 1) * cols] for i in range(n)]
        return lax.optimization_barrier(jnp.concatenate(pieces, axis=1)).astype(jnp.float32)

    weights_new, first_new, second_new = adam_update(owned(0), owned(1), owned(2), gradient)
    rounded = weights_new.astype(jnp.bfloat16)
    weights_bf16 = gather_line(rounded, length)
    return (weights_new, first_new, second_new, weights_bf16)


LANE = 128


def fsdp_kernel(
    n, parts, sizes, batches, relays, order, act, cot, w_in, m_in, v_in, w_out, m_out, v_out, b_out,
    raw, give_t, at_buf, c_buf, st_in, st_out, fin, stg, up, dn, tmp, old, wb,
    raw_sem, loc_sem, st_sem, own_sem, give_s, give_r, cot_s, cot_r,
    t_send, t_recv, fin_s, fin_r, stg_s, stg_r, fwd_s, fwd_r,
    up_s, up_r, dn_s, dn_r, y_send, y_recv, r_send, r_recv, l_send, l_recv, x_send, x_recv,
):
    f = lax.axis_index("fsdp")
    t = lax.axis_index("tensor")
    z, p = f // 2, f % 2
    length = n // 2
    last = length - 1
    tok, width = act.shape
    rows, cols = at_buf.shape[2], w_in.shape[0]
    pair = f + 1 - 2 * p
    bits = [1 << i for i in range(parts.bit_length() - 1)][::-1]
    starts = [sum(sizes[:k]) for k in range(len(sizes))]

    def copy(src, dst, send, recv, axis, target):
        return pltpu.make_async_remote_copy(
            src_ref=src, dst_ref=dst, send_sem=send, recv_sem=recv,
            device_id={axis: target}, device_id_type=pl.DeviceIdType.MESH,
        )

    def crossed(i, b):
        return i + b - 2 * b * ((t // b) % 2)

    def ring(j):
        return (z + j) % length

    def span(k):
        return pl.ds(starts[k], sizes[k])

    def lanes(i, size):
        return pl.ds(pl.multiple_of(i * size, size), size)

    def feature(q):
        return lanes(q, rows)

    raw_copies = [
        pltpu.make_async_copy(act.at[:, feature(q)], raw.at[i], raw_sem.at[i])
        for i, q in enumerate((1 - p, p))
    ]
    for c in raw_copies:
        c.start()
    here = pltpu.make_async_copy(cot, c_buf.at[0], loc_sem)
    here.start()

    firsts = [sum(batches[:i]) for i in range(len(batches))]

    def batch(i):
        return pl.ds(firsts[i], batches[i])

    def load_state(i, u, slot):
        d = 2 * ring(u + 1) + (p + 1 + u // length) % 2
        at = pl.ds(pl.multiple_of(d * rows + firsts[i], LANE), batches[i])
        return [
            pltpu.make_async_copy(
                src.at[:, at], st_in.at[slot, a, :, pl.ds(0, batches[i])], st_sem.at[slot, a]
            )
            for a, src in enumerate((w_in, m_in, v_in))
        ]

    for c in load_state(0, 0, 0):
        c.start()

    barrier = pltpu.get_barrier_semaphore()

    def greet(axis, target):
        pl.semaphore_signal(
            barrier, inc=1, device_id={axis: target}, device_id_type=pl.DeviceIdType.MESH
        )

    greet("fsdp", pair)
    for j in range(1, length):
        greet("fsdp", 2 * ring(j) + p)
    for b in bits:
        greet("tensor", crossed(t, b))
    pl.semaphore_wait(barrier, length + len(bits))

    head = tok // 4

    def cot_copy(i):
        at = pl.ds(0, head) if i == 0 else pl.ds(head, tok - head)
        return copy(cot.at[at], c_buf.at[1, at], cot_s.at[i], cot_r.at[i], "fsdp", pair)

    def turn(src, dst):
        def tile(r, carry):
            dst[lanes(r, LANE), :] = src[:, lanes(r, LANE)].T
            return carry

        lax.fori_loop(0, rows // LANE, tile, 0)

    def block_copy(which, i, h):
        return copy(
            at_buf.at[which, h], at_buf.at[which, h], t_send.at[which, i, h],
            t_recv.at[which, h], "tensor", crossed(t, bits[i]),
        )

    def held(i):
        found = [t]
        for b in bits[:i]:
            found = found + [crossed(h, b) for h in found]
        return found

    def spread_own(which):
        for i in range(len(bits)):
            block_copy(which, i, t).start()

    def spread_round(which, i):
        for h in held(i):
            g = crossed(h, bits[i])
            block_copy(which, i, g).wait_recv()
            for j in range(i + 1, len(bits)):
                block_copy(which, j, g).start()

    def spread_done(which):
        for i in range(len(bits)):
            for h in held(i):
                block_copy(which, i, h).wait_send()

    def fin_copy(i, zs, zd):
        return copy(
            st_out.at[2 * zd + p, :, batch(i)], fin.at[2 * zs + p, :, batch(i)],
            fin_s.at[i, zd], fin_r.at[i, zs], "fsdp", 2 * zd + p,
        )

    def stg_copy(i, zs, zd):
        return copy(
            st_out.at[2 * zd + 1 - p, :, batch(i)], stg.at[zs, :, batch(i)],
            stg_s.at[i, zd], stg_r.at[i, zs], "fsdp", 2 * zd + p,
        )

    def pack(i, u, carry):
        slot = u % 2

        @pl.when(u + 1 < n)
        def _():
            for c in load_state(i, u + 1, (u + 1) % 2):
                c.start()

        for c in load_state(i, u, slot):
            c.wait()
        zd, q = ring(u + 1), (p + 1 + u // length) % 2
        d = 2 * zd + q
        for a in range(3):
            st_out[d, a * cols : (a + 1) * cols, batch(i)] = st_in[
                slot, a, :, : batches[i]
            ].astype(jnp.bfloat16)

        @pl.when(d == f)
        def _():
            fin[d, :, batch(i)] = st_out[d, :, batch(i)]

        @pl.when((zd != z) & (q == p))
        def _():
            fin_copy(i, z, zd).start()

        @pl.when((zd != z) & (q != p))
        def _():
            stg_copy(i, z, zd).start()

        return carry

    cot_copy(0).start()
    for i in range(len(batches)):
        if i:
            for c in load_state(i, 0, 0):
                c.start()
        lax.fori_loop(0, n, functools.partial(pack, i), 0)

    raw_copies[0].wait()
    turn(raw.at[0], give_t)
    give = copy(give_t, at_buf.at[1, t], give_s, give_r, "fsdp", pair)
    give.start()
    cot_copy(1).start()
    raw_copies[1].wait()
    turn(raw.at[1], at_buf.at[0, t])
    spread_own(0)

    for i in range(len(bits)):
        spread_round(0, i)
    give.wait_recv()
    spread_own(1)
    for i in range(len(bits)):
        spread_round(1, i)
    here.wait()
    for i in range(2):
        cot_copy(i).wait_recv()

    def forward(i, zs, src=None):
        src = stg.at[zs, :, batch(i)] if src is None else src
        return copy(
            src, fin.at[2 * zs + p, :, batch(i)], fwd_s.at[i, zs], fwd_r.at[i, zs], "fsdp", pair
        )

    def forward_state(j, i):
        if j:
            zs = ring(length - j)
            stg_copy(i, zs, z).wait_recv()
            forward(i, zs).start()
        else:
            forward(i, z, st_out.at[pair, :, batch(i)]).start()

    def state_here(i):
        for j in range(1, length):
            fin_copy(i, ring(j), z).wait_recv()
        for zs in range(length):
            got = fin.at[2 * zs + 1 - p, :, batch(i)]
            forward_here = copy(got, got, fwd_s.at[i, zs], fwd_r.at[i, zs], "fsdp", pair)
            forward_here.wait_recv()

    def term(d, k):
        def tile(i, carry):
            at = lanes(i, width // 2)
            tmp[: sizes[k], at] = sum(
                jnp.dot(
                    at_buf[b, d, span(k), :], c_buf[b, :, at],
                    preferred_element_type=jnp.float32,
                )
                for b in range(2)
            )
            return carry

        lax.fori_loop(0, 2, tile, 0)

    def send_up(k, s):
        slot = s - jnp.minimum(z, 1)
        return copy(
            up.at[slot, span(k)], up.at[s, span(k)], up_s.at[k, s], up_r.at[k, s], "fsdp", f + 2
        )

    def send_dn(k, s):
        slot = s - jnp.minimum(last - z, 1)
        return copy(
            dn.at[slot, span(k)], dn.at[s, span(k)], dn_s.at[k, s], dn_r.at[k, s], "fsdp", f - 2
        )

    def take_up(k, s):
        got = up.at[s, span(k)]
        copy(got, got, up_s.at[k, s], up_r.at[k, s], "fsdp", f - 2).wait_recv()

    def take_dn(k, s):
        got = dn.at[s, span(k)]
        copy(got, got, dn_s.at[k, s], dn_r.at[k, s], "fsdp", f + 2).wait_recv()

    def add_in(ref, k, slot, first):
        mine = pl.ds(0, sizes[k])

        @pl.when(first)
        def _():
            ref[slot, span(k), :] = tmp[mine, :].astype(jnp.bfloat16)

        @pl.when(jnp.logical_not(first))
        def _():
            total = tmp[mine, :] + ref[slot, span(k), :].astype(jnp.float32)
            ref[slot, span(k), :] = total.astype(jnp.bfloat16)

    def reduce_step(k, s):
        @pl.when(z <= s)
        def _():
            term(last + z - s, k)
            if s:

                @pl.when(z > 0)
                def _():
                    take_up(k, s - 1)

            add_in(up, k, s - jnp.minimum(z, 1), z == 0)
            send_up(k, s).start()

        @pl.when(z >= last - s)
        def _():
            term(s - last + z, k)
            if s:

                @pl.when(z < last)
                def _():
                    take_dn(k, s - 1)

            add_in(dn, k, s - jnp.minimum(last - z, 1), z == last)
            send_dn(k, s).start()

    sub = LANE // 2

    arrived = []

    def adam(k):
        term(z, k)
        for i in range(len(batches)):
            if i not in arrived and firsts[i] < starts[k] + sizes[k]:
                state_here(i)
                arrived.append(i)

        inset = starts[k] % LANE
        if not inset:
            at = pl.ds(starts[k], LANE)
            for a in range(3):
                parts_of = [fin[src, a * cols : (a + 1) * cols, at] for src in range(n)]
                old[a] = jnp.concatenate(parts_of, axis=0).T
        mine = pl.ds(0, sizes[k])

        @pl.when(z > 0)
        def _():
            take_up(k, last - 1)
            tmp[mine, :] += up[last - 1, span(k), :].astype(jnp.float32)

        @pl.when(z < last)
        def _():
            take_dn(k, last - 1)
            tmp[mine, :] += dn[last - 1, span(k), :].astype(jnp.float32)

        def piece(j, carry):
            to = lanes(starts[k] // sub + j, sub)
            at = lanes(j, sub)
            was = pl.ds(pl.multiple_of(inset + j * sub, sub), sub)
            held_now = [old[a, was, :].astype(jnp.float32) for a in range(3)]
            new = adam_update(*held_now, tmp[at, :])
            for a, out in enumerate((w_out, m_out, v_out)):
                out[to, :] = new[a]
            wb[to, :] = new[0].astype(jnp.bfloat16)
            return carry

        lax.fori_loop(0, sizes[k] // sub, piece, 0)
        gather_start(k)

    def block(c, q, k):
        return b_out.at[pl.ds(pl.multiple_of((2 * c + q) * rows + starts[k], LANE // 2), sizes[k])]

    def to_pair(k, c, src=None):
        src = block(c, p, k) if src is None else src
        return copy(src, block(c, p, k), y_send.at[k, c], y_recv.at[k, c], "fsdp", pair)

    def to_right(k, s, src=None):
        src = block(z - s, p, k) if src is None else src
        return copy(src, block(z - s, p, k), r_send.at[k, s], r_recv.at[k, s], "fsdp", f + 2)

    def to_left(k, s, src=None):
        src = block(z + s, p, k) if src is None else src
        return copy(src, block(z + s, p, k), l_send.at[k, s], l_recv.at[k, s], "fsdp", f - 2)

    def keep(k):
        return pltpu.make_async_copy(wb.at[span(k)], block(z, p, k), own_sem.at[k])

    def gather_start(k):
        mine = wb.at[span(k)]
        to_pair(k, z, mine).start()

        @pl.when(z < last)
        def _():
            to_right(k, 0, mine).start()

        @pl.when(z > 0)
        def _():
            to_left(k, 0, mine).start()

        keep(k).start()

    even = z % 2 == 0
    beside = z + 1 - 2 * (z % 2)

    def relay(k):
        got = block(z, 1 - p, k)
        copy(got, got, y_send.at[k, z], y_recv.at[k, z], "fsdp", pair).wait_recv()
        relay_copy(k, z).start()

    def relay_copy(k, c):
        got = block(c, 1 - p, k)
        return copy(got, got, x_send.at[k], x_recv.at[k], "fsdp", 2 * beside + p)

    def onward(k, s, c, near):
        if s or k not in relays:
            to_pair(k, c).start()
        else:

            @pl.when(jnp.logical_not(near))
            def _():
                to_pair(k, c).start()

    def gather_step(k, s):
        @pl.when(z > s)
        def _():
            c = z - 1 - s
            got = block(c, p, k)
            copy(got, got, r_send.at[k, s], r_recv.at[k, s], "fsdp", f - 2).wait_recv()
            if s + 1 < last:

                @pl.when(z < last)
                def _():
                    to_right(k, s + 1).start()

            onward(k, s, c, z % 2 == 1)

        @pl.when(z < last - s)
        def _():
            c = z + 1 + s
            got = block(c, p, k)
            copy(got, got, l_send.at[k, s], l_recv.at[k, s], "fsdp", f + 2).wait_recv()
            if s + 1 < last:

                @pl.when(z > 0)
                def _():
                    to_left(k, s + 1).start()

            onward(k, s, c, even)


    forward_state(0, 0)
    for kind, *at in order:
        {
            "F": forward_state, "R": reduce_step, "A": adam, "G": gather_step, "X": relay,
        }[kind](*at)

    give.wait_send()
    for i in range(2):
        cot_copy(i).wait_send()
        spread_done(i)
    for i in range(len(batches)):
        for j in range(1, length):
            fin_copy(i, z, ring(j)).wait_send()
            stg_copy(i, z, ring(j)).wait_send()
        for zs in range(length):
            forward(i, zs).wait_send()
    for k in range(len(sizes)):
        keep(k).wait()
        for s in range(last):

            @pl.when(z <= s)
            def _():
                send_up(k, s).wait_send()

            @pl.when(z >= last - s)
            def _():
                send_dn(k, s).wait_send()

            @pl.when((z < last) & (z >= s))
            def _():
                to_right(k, s).wait_send()

            @pl.when((z > 0) & (last - z >= s))
            def _():
                to_left(k, s).wait_send()

        if k in relays:
            relay_copy(k, z).wait_send()
            relay_copy(k, beside).wait_recv()
            to_pair(k, z).wait_send()
            others = [ring(j) for j in range(1, length)]
        else:
            others = list(range(length))

        def settle(c):
            to_pair(k, c).wait_send()
            theirs = block(c, 1 - p, k)
            copy(theirs, theirs, y_send.at[k, c], y_recv.at[k, c], "fsdp", pair).wait_recv()

        for c in others:
            if k in relays:
                pl.when(c != beside)(functools.partial(settle, c))
            else:
                settle(c)


TUNED = (
    "F21 F31 F10 R00",
    "F30 F11 R10 R20",
    "R01 R11 R21 F20",
    "R02 R12 F01 R22",
    "A0 A1 A2 G00",
    "G10 G20 G01 R30",
    "R31 G11 R50 R40",
    "G21 G02 R41 G12",
    "R32 R51 R42 G22",
    "A3 A4 R52 G40",
    "G30 A5 G41 G31",
    "G50 G42 X5 G32",
    "G51 X2 G52",
)
RELAYS = (2, 5)
FIRST_BATCH = 1


def step_order(chunks, last):
    tiles = chunks - 1
    if (tiles, last) == (5, 3):
        order = [(w[0], *(int(c) for c in w[1:])) for w in " ".join(TUNED).split()]
        first = FIRST_BATCH
        return tuple(order), RELAYS, (first, tiles - first)
    order = [("F", j + 1, 0) for j in range(last)]
    for k in range(chunks):
        order += [("R", k, s) for s in range(last)] + [("A", k)]
        order += [("G", k, s) for s in range(last)]
    return tuple(order), (), (tiles,)


def fast_body(activations, cotangent, weights, first_moment, second_moment, *, n, parts):
    depth, cols = weights.shape
    tok, width = activations.shape
    rows = depth // n
    length = n // 2
    sizes = (LANE,) * (rows // LANE - 1) + (LANE // 2,) * 2
    chunks = len(sizes)
    order, relays, batches = step_order(chunks, length - 1)
    batches = tuple(b * LANE for b in batches)
    rounds = parts.bit_length() - 1
    dma = pltpu.SemaphoreType.DMA
    half, full = jnp.bfloat16, jnp.float32
    hops = max(length - 1, 1)
    row = pltpu.VMEM((rows, width), full)
    anywhere = pl.BlockSpec(memory_space=pl.ANY)
    return tuple(
        pl.pallas_call(
            functools.partial(fsdp_kernel, n, parts, sizes, batches, relays, order),
            out_shape=(row, row, row, jax.ShapeDtypeStruct((depth, width), half)),
            in_specs=[anywhere] * 5,
            out_specs=(pl.BlockSpec(memory_space=pltpu.VMEM),) * 3 + (anywhere,),
            scratch_shapes=[
                pltpu.VMEM((2, tok, rows), half),
                pltpu.VMEM((rows, tok), half),
                pltpu.VMEM((2, parts, rows, tok), half),
                pltpu.VMEM((2, tok, width), half),
                pltpu.VMEM((2, 3, cols, rows), full),
                pltpu.VMEM((n, 3 * cols, rows), half),
                pltpu.VMEM((n, 3 * cols, rows), half),
                pltpu.VMEM((length, 3 * cols, rows), half),
                pltpu.VMEM((hops, rows, width), half),
                pltpu.VMEM((hops, rows, width), half),
                pltpu.VMEM((max(sizes), width), full),
                pltpu.VMEM((3, max(sizes), width), half),
                pltpu.VMEM((rows, width), half),
                dma((2,)), dma, dma((2, 3)), dma((chunks,)),
                dma, dma, dma((2,)), dma((2,)),
                dma((2, rounds, parts)), dma((2, parts)),
            ]
            + [dma((len(batches), length))] * 6
            + [dma((chunks, hops))] * 4
            + [dma((chunks, length))] * 2
            + [dma((chunks, hops))] * 4
            + [dma((chunks,))] * 2,
            compiler_params=pltpu.CompilerParams(
                collective_id=0, has_side_effects=True, vmem_limit_bytes=54 * 2**20
            ),
            name="fsdp_step",
        )(activations, cotangent, weights.T, first_moment.T, second_moment.T)
    )


def solution(mesh):
    n, parts = mesh.shape["fsdp"], mesh.shape["tensor"]

    def run(*arrays):
        rows, width = arrays[2].shape[0] // n, arrays[0].shape[1]
        fits = rows % LANE == 0 and n == 2 * parts and width == 2 * rows
        if fits and arrays[2].shape[1] % 16 == 0 and parts & (parts - 1) == 0:
            return fast_body(*arrays, n=n, parts=parts)
        return body(*arrays, n=n, parts=parts)

    return jax.shard_map(
        run,
        mesh=mesh,
        in_specs=(
            P("fsdp", "tensor"),
            P("fsdp", "tensor"),
            P(None, ("tensor", "fsdp")),
            P(None, ("tensor", "fsdp")),
            P(None, ("tensor", "fsdp")),
        ),
        out_specs=(
            P("fsdp", "tensor"),
            P("fsdp", "tensor"),
            P("fsdp", "tensor"),
            P(None, "tensor"),
        ),
        check_vma=False,
    )
```
